256 devices in a mesh: seq: 64 (over x_hi, z, y), tp: 4 (over x_lo, core).
Axes of the slice: x: 4 (x_hi: 2, x_lo: 2; x = x_hi * 2 + x_lo), y: 4, z: 8, core: 2. Of those that a mesh axis runs over, the one named last changes fastest.
Arguments:
- hidden: bfloat16 [8192, 4096], P('seq', 'tp'), may hold values from -6 to 6
- w_proj: bfloat16 [4096, 1024], P('tp'), may hold values from -1 to 1
- codes: int32 [8192, 4], P('seq'), may hold values from 0 to 2047
- embed_table: bfloat16 [3, 2048, 1024], P(None, None, 'tp'), may hold values from -6 to 6
- w_qkv: bfloat16 [1024, 3, 1024], P(None, None, 'tp'), may hold values from -1 to 1
- w_out: bfloat16 [1024, 1024], P('tp'), may hold values from -0.1875 to 0.1875
- head_table: bfloat16 [4, 1024, 2048], P(None, None, 'tp'), may hold values from -1 to 1
- gain_attn: float32 [1024], replicated, may hold values from 0.5 to 1.5
- gain_head: float32 [1024], replicated, may hold values from 0.5 to 1.5
Outputs:
- row_loss: float32 [8192, 4], P('seq')
- grad_hidden: bfloat16 [8192, 4096], P('seq', 'tp')
- grad_proj: float32 [4096, 1024], P('tp', 'seq')
The draws below stay inside these ranges and needn't reach their ends.
All inputs are finite; a program needn't handle non-finite values.
Results may differ from the reference program's by a relative error of at most 0.02.
Values may be sent and summed in bfloat16 or wider, within the bound.
A program may use at most 64 MiB of HBM per device.

```python
import jax
import jax.numpy as jnp
from jax import lax

DT = 4096
DD = 1024
V = 2048
HEADS = 16
KW = 4
FRAMES = 8192


def draw_hidden(key, part):
    drawn = jax.random.truncated_normal(jax.random.fold_in(key, 1), -6.0, 6.0, (FRAMES, DT), jnp.float32)
    return drawn.astype(jnp.bfloat16)


def draw_w_proj(key, part):
    spread = DT ** (-0.5)
    drawn = jax.random.truncated_normal(jax.random.fold_in(key, 11), -6.0, 6.0, (DT, DD), jnp.float32) * spread
    return drawn.astype(jnp.bfloat16)


def draw_w_qkv(key, part):
    spread = DD ** (-0.5)
    drawn = jax.random.truncated_normal(jax.random.fold_in(key, 21), -6.0, 6.0, (DD, 3, DD), jnp.float32) * spread
    return drawn.astype(jnp.bfloat16)


def draw_head_table(key, part):
    spread = (DD // 9) ** (-0.5)
    drawn = jax.random.truncated_normal(jax.random.fold_in(key, 31), -6.0, 6.0, (KW, DD, V), jnp.float32) * spread
    return drawn.astype(jnp.bfloat16)


def plant(values, key, smallest, top_value):
    place = [jax.random.randint(jax.random.fold_in(key, axis), (), 0, length) for axis, length in enumerate(values.shape)]
    longest = values.shape.index(max(values.shape))
    beside = place[:longest] + [(place[longest] + 1) % values.shape[longest]] + place[longest + 1:]
    return values.at[tuple(place)].set(smallest).at[tuple(beside)].set(top_value)


def block_scale(own_key, extent, pieces, smallest, largest):
    factor_of = 1.0
    for dim, blocks in pieces:
        steps = jax.random.uniform(jax.random.fold_in(jax.random.fold_in(own_key, 6), dim), (blocks,), jnp.float32, smallest / len(pieces), largest / len(pieces))
        factor_of = factor_of * jnp.repeat(jnp.exp(steps), extent[dim] // blocks).reshape((-1,) + (1,) * (len(extent) - 1 - dim))
    return factor_of


def bell_draw(rng, shape, deviation, most, pieces=(), held_as=jnp.bfloat16):
    entries = jax.random.normal(rng, shape, jnp.float32) * deviation
    if len(pieces) > 0:
        entries = block_scale(rng, shape, pieces, -0.22, 0.18) * entries
    return jnp.clip(entries, min=-most, max=most).astype(held_as)


def setup_inputs(seed: int = 0) -> dict:
    splits = jax.random.split(jax.random.key(seed), 10)
    return {
        "hidden": draw_hidden(jax.random.fold_in(splits[9], 71), 0),
        "w_proj": draw_w_proj(jax.random.fold_in(splits[9], 71), 0),
        "codes": plant(jax.random.randint(splits[2], (FRAMES, KW), 0, V), jax.random.fold_in(splits[2], 1), 0, V - 1).astype(jnp.int32),
        "embed_table": bell_draw(splits[3], (KW - 1, V, DD), 1.0, 6.0, ((2, 4),)),
        "w_qkv": draw_w_qkv(jax.random.fold_in(splits[9], 71), 0),
        "w_out": bell_draw(splits[5], (DD, DD), DD ** -0.5, 0.1875, ((0, 4),)),
        "head_table": draw_head_table(jax.random.fold_in(splits[9], 71), 0),
        "gain_attn": jnp.clip(1.0 + 0.1 * jax.random.normal(splits[7], (DD,), jnp.float32), 0.5, 1.5),
        "gain_head": jnp.clip(1.0 + 0.1 * jax.random.normal(splits[8], (DD,), jnp.float32), 0.5, 1.5),
    }


def rms_norm(stream, gain):
    return stream * lax.rsqrt(lax.optimization_barrier(jnp.mean(stream * stream, axis=-1, keepdims=True)) + 1e-06) * gain

def norm_back(stream, gain, cotangent):
    return jax.vjp(lambda value: rms_norm(value, gain), stream)[1](cotangent)[0]

def attend(query, keys, values):
    scale = query.shape[-1] ** (-0.5)
    count = query.shape[1]
    scores = jnp.einsum('fqhd,fkhd->fhqk', query.astype(jnp.float32), keys.astype(jnp.float32)) * scale
    causal = jnp.arange(count)[:, None] >= jnp.arange(count)[None, :]
    scores = jnp.where(causal, scores, -1e+30)
    shifted = jnp.exp(scores - lax.optimization_barrier(jnp.max(scores, axis=-1, keepdims=True)))
    weights = shifted / lax.optimization_barrier(jnp.sum(shifted, axis=-1, keepdims=True))
    weights_low = weights.astype(jnp.bfloat16)
    attended = jnp.einsum('fhqk,fkhd->fqhd', weights_low.astype(jnp.float32), values.astype(jnp.float32)).astype(jnp.bfloat16)
    return (attended, weights, weights_low)

def attend_back(query, keys, values, weights, weights_low, attended_grad):
    scale = query.shape[-1] ** (-0.5)
    grad_f = attended_grad.astype(jnp.float32)
    prob_grad = jnp.einsum('fqhd,fkhd->fhqk', grad_f, values.astype(jnp.float32))
    score_grad = (weights * (prob_grad - lax.optimization_barrier(jnp.sum(weights * prob_grad, axis=-1, keepdims=True))) * scale).astype(jnp.bfloat16)
    score_f = score_grad.astype(jnp.float32)
    query_grad = jnp.einsum('fhqk,fkhd->fqhd', score_f, keys.astype(jnp.float32)).astype(jnp.bfloat16)
    key_grad = jnp.einsum('fhqk,fqhd->fkhd', score_f, query.astype(jnp.float32)).astype(jnp.bfloat16)
    value_grad = jnp.einsum('fhqk,fqhd->fkhd', weights_low.astype(jnp.float32), grad_f).astype(jnp.bfloat16)
    return jnp.stack([query_grad, key_grad, value_grad], axis=2)

def reference(hidden, w_proj, codes, embed_table, w_qkv, w_out, head_table, gain_attn, gain_head):
    frames = hidden.shape[0]
    width = w_proj.shape[1]
    head_dim = width // HEADS
    total = float(frames * KW)
    context = jnp.dot(hidden, w_proj, preferred_element_type=jnp.float32)
    looked = jnp.stack([jnp.take(embed_table[column], codes[:, column], axis=0) for column in range(KW - 1)], axis=1)
    shifted_in = jnp.concatenate([jnp.zeros((frames, 1, width), jnp.float32), looked.astype(jnp.float32)], axis=1)
    stream_in = context[:, None, :] + shifted_in
    normed_in = rms_norm(stream_in, gain_attn).astype(jnp.bfloat16)
    projected = jnp.dot(normed_in.reshape(-1, width), w_qkv.reshape(width, -1), preferred_element_type=jnp.float32)
    projected = projected.astype(jnp.bfloat16).reshape(frames, KW, 3, HEADS, head_dim)
    query, keys, values = (projected[:, :, 0], projected[:, :, 1], projected[:, :, 2])
    attended, weights, weights_low = attend(query, keys, values)
    mixed = jnp.dot(attended.reshape(-1, width), w_out, preferred_element_type=jnp.float32)
    stream_mid = stream_in + mixed.reshape(frames, KW, width)
    normed_out = rms_norm(stream_mid, gain_head).astype(jnp.bfloat16)
    logits = jnp.einsum('fkd,kdv->fkv', normed_out.astype(jnp.float32), head_table.astype(jnp.float32))
    hits = codes[..., None] == jnp.arange(logits.shape[-1], dtype=jnp.int32)
    top = lax.optimization_barrier(jnp.max(logits, axis=-1))
    exp_total = lax.optimization_barrier(jnp.sum(jnp.exp(logits - top[..., None]), axis=-1))
    log_total = top + jnp.log(exp_total)
    target = lax.optimization_barrier(jnp.sum(jnp.where(hits, logits, 0.0), axis=-1))
    row_loss = log_total - target
    logit_grad = ((jnp.exp(logits - log_total[..., None]) - hits.astype(jnp.float32)) / total).astype(jnp.bfloat16)
    normed_grad = jnp.einsum('fkv,kdv->fkd', logit_grad.astype(jnp.float32), head_table.astype(jnp.float32))
    mid_grad = norm_back(stream_mid, gain_head, normed_grad)
    mid_low = mid_grad.astype(jnp.bfloat16)
    attended_grad = jnp.dot(mid_low.reshape(-1, width), w_out.T, preferred_element_type=jnp.float32)
    attended_grad = attended_grad.astype(jnp.bfloat16).reshape(frames, KW, HEADS, head_dim)
    qkv_grad = attend_back(query, keys, values, weights, weights_low, attended_grad)
    normin_grad = jnp.dot(qkv_grad.reshape(frames * KW, -1), w_qkv.reshape(width, -1).T, preferred_element_type=jnp.float32)
    stream_grad = mid_grad + norm_back(stream_in, gain_attn, normin_grad.reshape(frames, KW, width))
    context_grad = lax.optimization_barrier(jnp.sum(stream_grad, axis=1)).astype(jnp.bfloat16)
    grad_hidden = jnp.dot(context_grad, w_proj.T, preferred_element_type=jnp.float32).astype(jnp.bfloat16)
    grad_proj = jnp.dot(hidden.T, context_grad, preferred_element_type=jnp.float32)
    return (row_loss, grad_hidden, grad_proj)
```

```python
import functools

import jax
import jax.numpy as jnp
from jax import lax
from jax.experimental import pallas as pl
from jax.experimental.pallas import tpu as pltpu
from jax.sharding import PartitionSpec as P

HEADS = 16
KW = 4
TP = 4
EPS = 1e-06
RB = 32
F32 = jnp.float32
BF16 = jnp.bfloat16
MESH = pl.DeviceIdType.MESH
LAYOUT = {64: (2, 8, 4), 4: (1, 2, 2), 1: (1, 1, 1)}


def mm(a, b):
    return jnp.dot(a, b, preferred_element_type=F32)


def mm_t(a, b):
    return lax.dot_general(a, b, (((1,), (1,)), ((), ())), preferred_element_type=F32)


def remote(src, dst, send, recv, device):
    return pltpu.make_async_remote_copy(
        src_ref=src, dst_ref=dst, send_sem=send, recv_sem=recv, device_id=device, device_id_type=MESH
    )


def kernel(
    seq_size,
    hid_h, wproj_h, codes_h, emb_h, wqkv_h, wo_h, head_h, ga_h, gh_h,
    loss_o, ghid_o, gproj_o,
    hg, wproj, codes, emb, wqkv, wo, head, ga, gh,
    ccol, looked, c_s, c_r, c_2, s_in, s_mid, normed, q, k, v, wts, att, bd,
    big, g12, st_c, st, sc, midsum, b_s, b_r, b_s2, b_r2, ag, dkv, dqkv,
    e_s, e_r, e_2, cg, tsend, trecv, psend, precv, part,
    lsem, hid_ss, hid_rs, wo_ss, wo_rs, lk_ss, lk_rs, c_ss, c_rs, att_ss, att_rs,
    st_ss, st_rs, b_ss, b_rs, e_ss, e_rs, t_ss, t_rs, p_ss, p_rs,
):
    xs, zs, ys = LAYOUT[seq_size]
    zb_n = min(2, zs)
    zh_n = zs // zb_n
    npos, nsg = zb_n * ys, xs * zh_n
    cw = 1024 // seq_size
    total = float(128 * seq_size * KW)

    r = lax.axis_index("tp")
    s = lax.axis_index("seq")
    core = r % 2
    chip = r // 2
    p = chip * 2 + (1 - core)
    x = (1 - chip) * 2 + core
    d = (1 - chip) * 2 + (1 - core)
    y = s % ys
    z = (s // ys) % zs
    xh = s // (ys * zs)
    pos = (z % zb_n) * ys + y
    sg = xh * zh_n + z // zb_n
    to_p, to_x, to_d = {"tp": p}, {"tp": x}, {"tp": d}
    flip = {"seq": (xs - 1 - xh) * (ys * zs) + z * ys + y, "tp": x}

    def seq_of(position, supergroup):
        yy, zb = position % ys, position // ys
        zh, xx = supergroup % zh_n, supergroup // zh_n
        return xx * (ys * zs) + (zh * zb_n + zb) * ys + yy

    pos_peers = [lax.rem(pos + i, npos) for i in range(1, npos)]
    sg_peers = [lax.rem(sg + i, nsg) for i in range(1, nsg)]

    def load(src, dst, i):
        copy = pltpu.make_async_copy(src, dst, lsem.at[i])
        copy.start()
        return copy

    l_hid = load(hid_h, hg.at[pos], 0)
    l_wproj = load(wproj_h, wproj, 1)
    l_codes = load(codes_h, codes, 2)
    l_emb = [load(emb_h.at[i], emb.at[i], 3 + i) for i in range(3)]
    l_ga = load(ga_h, ga, 6)
    l_gh = load(gh_h, gh, 7)
    l_qkv = load(wqkv_h, wqkv, 8)
    l_wo = load(wo_h, wo.at[r], 9)
    l_head = load(head_h, head, 10)

    barrier = pltpu.get_barrier_semaphore()
    peers = [to_p, to_x, to_d]
    if xs > 1:
        peers.append(flip)
    peers += [{"seq": seq_of(i, sg)} for i in pos_peers]
    peers += [{"seq": seq_of(pos, i)} for i in sg_peers]
    for peer in peers:
        pl.semaphore_signal(barrier, inc=1, device_id=peer, device_id_type=MESH)

    l_hid.wait()
    l_wproj.wait()
    mine = pl.ds(pl.multiple_of(core * 512, 512), 512)
    other = pl.ds(pl.multiple_of((1 - core) * 512, 512), 512)
    c_s[...] = mm(hg[pos], wproj[:, other]).astype(BF16)

    l_codes.wait()
    st_c[...] = jnp.zeros_like(st_c)
    st_c[0:KW, :] = codes[...].astype(F32)
    code_cols = st_c[...].T
    for i in range(KW):
        ccol[i] = jnp.broadcast_to(code_cols[:, i : i + 1], (128, 128)).astype(jnp.int32)

    pl.semaphore_wait(barrier, len(peers))

    c1 = remote(c_s, c_r, c_ss.at[0], c_rs.at[0], to_p)
    c1.start()

    w_p = remote(wo_h, wo.at[r], wo_ss.at[0], wo_rs.at[r], to_p)
    w_x = remote(wo_h, wo.at[r], wo_ss.at[1], wo_rs.at[r], flip if xs > 1 else to_x)
    w_p.start()
    w_x.start()

    lane = lax.broadcasted_iota(jnp.int32, (128, 128), 1)
    looks = []

    def look(i):
        l_emb[i].wait()
        code = ccol[i]
        hot = jnp.concatenate(
            [(code == lane + 128 * g).astype(F32).astype(BF16) for g in range(16)], axis=1
        )
        looked[r, i] = mm(hot, emb[i]).astype(BF16)
        for n, to in enumerate((to_x, to_p)):
            copy = remote(looked.at[r, i], looked.at[r, i], lk_ss.at[i, n], lk_rs.at[i, r], to)
            copy.start()
            looks.append(copy)

    own_half = mm(hg[pos], wproj[:, mine])
    look(0)
    c1.wait_recv()
    c_2[chip, core] = (own_half + c_r[...].astype(F32)).astype(BF16)
    c2x = remote(c_2.at[chip, core], c_2.at[chip, core], c_ss.at[1], c_rs.at[1], to_x)
    c2p = remote(c_2.at[chip, core], c_2.at[chip, core], c_ss.at[2], c_rs.at[2], to_p)
    c2x.start()
    c2p.start()
    look(1)
    look(2)

    hids = []
    for n in range(1, ys):
        py = lax.rem(y + n, ys)
        copy = remote(hid_h, hg.at[pos], hid_ss.at[n - 1], hid_rs.at[pos], {"seq": seq_of((z % zb_n) * ys + py, sg)})
        copy.start()
        hids.append(copy)
    pos_z = (1 - z % zb_n) * ys + y
    if zb_n > 1:
        copy = remote(hid_h, hg.at[pos], hid_ss.at[3], hid_rs.at[pos], {"seq": seq_of(pos_z, sg)})
        copy.start()
        hids.append(copy)

    bd[...] = (
        lax.broadcasted_iota(jnp.int32, (256, 256), 0) // 64
        == lax.broadcasted_iota(jnp.int32, (256, 256), 1) // 64
    ).astype(F32).astype(BF16)

    relays = []

    def relay(buf, send, recv):
        copy = remote(buf, buf, send, recv, to_p)
        copy.start()
        relays.append(copy)

    def landed(buf, recv):
        remote(buf, buf, lsem.at[15], recv, to_p).wait_recv()

    landed(looked.at[x, 0], lk_rs.at[0, x])
    relay(looked.at[x, 0], lk_ss.at[0, 2], lk_rs.at[0, x + 4])
    landed(c_2.at[1 - chip, core], c_rs.at[1])
    relay(c_2.at[1 - chip, core], c_ss.at[3], c_rs.at[3])
    landed(looked.at[x, 1], lk_rs.at[1, x])
    relay(looked.at[x, 1], lk_ss.at[1, 2], lk_rs.at[1, x + 4])
    landed(c_2.at[chip, 1 - core], c_rs.at[2])
    landed(c_2.at[1 - chip, 1 - core], c_rs.at[3])
    l_ga.wait()

    def stream_rows(i, rb):
        rows = pl.ds(pl.multiple_of(rb * RB, RB), RB)
        ctx = jnp.concatenate(
            [c_2[0, h, rows, :].astype(F32) + c_2[1, h, rows, :].astype(F32) for h in range(2)], axis=1
        )
        if i > 0:
            ctx = ctx + jnp.concatenate([looked[j, i - 1, rows, :].astype(F32) for j in range(TP)], axis=1)
        s_in[i, rows, :] = ctx
        scale = lax.rsqrt(jnp.mean(ctx * ctx, axis=1, keepdims=True) + EPS)
        normed[i, rows, :] = (ctx * scale * ga[...]).astype(BF16)

    def project(i):
        for n, dst in enumerate((q, k, v)):
            dst[i] = mm(normed[i], wqkv[n]).astype(BF16)

    def attend(a):
        probe = [q[a].astype(F32) * k[b].astype(F32) for b in range(a + 1)]
        if a == 0:
            att[r, 0] = v[0]
        else:
            prod = jnp.concatenate(probe, axis=0)
            high = prod.astype(BF16)
            low = (prod - high.astype(F32)).astype(BF16)
            sums = (mm(high, bd[...]) + mm(low, bd[...])) * 0.125
            rows = [sums[b * 128 : (b + 1) * 128] for b in range(a + 1)]
            top = functools.reduce(jnp.maximum, rows)
            rows = [jnp.exp(row - top) for row in rows]
            inv = 1.0 / functools.reduce(jnp.add, rows)
            out = jnp.zeros((128, 256), F32)
            for b in range(a + 1):
                w = rows[b] * inv
                wts[a * (a + 1) // 2 + b] = w
                out = out + w.astype(BF16).astype(F32) * v[b].astype(F32)
            att[r, a] = out.astype(BF16)
        for n, to in enumerate((to_x, to_p)):
            copy = remote(att.at[r, a], att.at[r, a], att_ss.at[a, n], att_rs.at[a, r], to)
            copy.start()
            relays.append(copy)

    for i in range(KW):
        if i > 0:
            if i == 2:
                landed(looked.at[x, 2], lk_rs.at[2, x])
                relay(looked.at[x, 2], lk_ss.at[2, 2], lk_rs.at[2, x + 4])
            landed(looked.at[p, i - 1], lk_rs.at[i - 1, p])
            landed(looked.at[d, i - 1], lk_rs.at[i - 1, d + 4])
        lax.fori_loop(0, 128 // RB, lambda rb, c: (stream_rows(i, rb), c)[1], 0)
        if i == 0:
            l_qkv.wait()
        project(i)
        attend(i)

    if zb_n > 1:
        landed(hg.at[pos_z], hid_rs.at[pos_z])
        for n in range(1, ys):
            py = lax.rem(y + n, ys)
            copy = remote(hg.at[pos_z], hg.at[pos_z], hid_ss.at[3 + n], hid_rs.at[pos_z], {"seq": seq_of((z % zb_n) * ys + py, sg)})
            copy.start()
            hids.append(copy)
    landed(wo.at[x], wo_rs.at[x])
    relay(wo.at[x], wo_ss.at[2], wo_rs.at[x + 4])
    l_wo.wait()
    landed(wo.at[p], wo_rs.at[p])
    l_gh.wait()
    l_head.wait()
    st_c[...] = jnp.zeros_like(st_c)

    def forward(i, carry):
        landed(att.at[x, i], att_rs.at[i, x])
        copy = remote(att.at[x, i], att.at[x, i], att_ss.at[i, 2], att_rs.at[i, x + 4], to_p)
        copy.start()
        acc = s_in[i] + mm(att[r, i], wo[r])
        landed(att.at[p, i], att_rs.at[i, p])
        big[...] = acc + mm(att[p, i], wo[p]) + mm(att[x, i], wo[x])

        @pl.when(i == 0)
        def _():
            landed(wo.at[d], wo_rs.at[d + 4])

        landed(att.at[d, i], att_rs.at[i, d + 4])
        s_mid[i] = big[...] + mm(att[d, i], wo[d])

        def rows_of(rb, c):
            rows = pl.ds(pl.multiple_of(rb * RB, RB), RB)
            val = s_mid[i, rows, :]
            scale = lax.rsqrt(jnp.mean(val * val, axis=1, keepdims=True) + EPS)
            normed[i, rows, :] = (val * scale * gh[...]).astype(BF16)
            return c

        lax.fori_loop(0, 128 // RB, rows_of, 0)
        logits = mm(normed[i], head[i])
        code = ccol[i]
        hit = jnp.concatenate([code == lane + (128 * g + r * 512) for g in range(4)], axis=1)
        top = jnp.max(logits, axis=1, keepdims=True)
        grown = jnp.exp(logits - top)
        total_exp = jnp.sum(grown, axis=1, keepdims=True)
        target = jnp.sum(jnp.where(hit, logits, 0.0), axis=1, keepdims=True)
        st_c[...] = jnp.where(
            lane == i, top, jnp.where(lane == i + 8, total_exp, jnp.where(lane == i + 16, target, st_c[...]))
        )
        pair = jnp.concatenate(
            [jnp.where(hit, 0.0, grown).astype(BF16), hit.astype(F32).astype(BF16)], axis=0
        )
        g12[i] = mm_t(pair, head[i])
        copy.wait_send()
        return carry

    lax.fori_loop(0, KW, forward, 0)

    st[r] = st_c[...].T[0:24, :]
    stats = []
    for n, to in enumerate((to_p, to_x, to_d)):
        copy = remote(st.at[r], st.at[r], st_ss.at[n], st_rs.at[r], to)
        copy.start()
        stats.append(copy)
    for slot in (p, x, d):
        landed(st.at[slot], st_rs.at[slot])
    tops = [st[j, 0:8, :] for j in range(TP)]
    top = functools.reduce(jnp.maximum, tops)
    exp_total = functools.reduce(jnp.add, [st[j, 8:16, :] * jnp.exp(tops[j] - top) for j in range(TP)])
    target = functools.reduce(jnp.add, [st[j, 16:24, :] for j in range(TP)])
    log_total = top + jnp.log(exp_total)
    loss_o[...] = (log_total - target)[0:KW, :]
    sc[...] = jnp.zeros_like(sc)
    sc[0:8, :] = jnp.exp(st[r, 0:8, :] - log_total) * (1.0 / total)
    sc[8:16, :] = (jnp.exp(target - log_total) - 1.0) * (1.0 / total)
    sc[...] = sc[...].T
    midsum[...] = jnp.zeros_like(midsum)

    def send_on(i):
        landed(b_r.at[i], b_rs.at[i, 0])
        b_s2[i] = (ag[i, 1] + b_r[i, 1].astype(F32)).astype(BF16)
        remote(b_s2.at[i], b_r2.at[i], b_ss.at[i, 1], b_rs.at[i, 1], to_x).start()

    def head_back(n, carry):
        i = KW - 1 - n

        def rows_of(rb, c):
            start = pl.multiple_of(rb * RB, RB)
            rows = pl.ds(start, RB)
            ln = lax.broadcasted_iota(jnp.int32, (RB, 128), 1)
            both = sc[rows, :]
            grow = jnp.sum(jnp.where(ln == i, both, 0.0), axis=1, keepdims=True)
            hot = jnp.sum(jnp.where(ln == i + 8, both, 0.0), axis=1, keepdims=True)
            val = s_mid[i, rows, :]
            cot = (grow * g12[i, rows, :] + hot * g12[i, pl.ds(pl.multiple_of(128 + start, RB), RB), :]) * gh[...]
            scale = lax.rsqrt(jnp.mean(val * val, axis=1, keepdims=True) + EPS)
            along = jnp.mean(cot * val, axis=1, keepdims=True) * (scale * scale * scale)
            back = cot * scale - val * along
            midsum[rows, :] = midsum[rows, :] + back
            normed[i, rows, :] = back.astype(BF16)
            return c

        lax.fori_loop(0, 128 // RB, rows_of, 0)
        low = normed[i]
        b_s[i, 0] = mm_t(low, wo[p]).astype(BF16)
        b_s[i, 1] = mm_t(low, wo[d]).astype(BF16)
        remote(b_s.at[i], b_r.at[i], b_ss.at[i, 0], b_rs.at[i, 0], to_p).start()
        ag[i, 1] = mm_t(low, wo[x])
        ag[i, 0] = mm_t(low, wo[r])

        @pl.when(n > 0)
        def _():
            send_on(i + 1)

        return carry

    lax.fori_loop(0, KW, head_back, 0)
    send_on(0)

    for a in range(KW - 1, -1, -1):
        landed(b_r2.at[a], b_rs.at[a, 1])
        out_grad = (ag[a, 0] + b_r[a, 0].astype(F32) + b_r2[a].astype(F32)).astype(BF16).astype(F32)
        if a == 0:
            dq = jnp.zeros((128, 256), F32)
            dk = dkv[0, 0]
            dv = dkv[1, 0] + out_grad
        else:
            prod = jnp.concatenate([out_grad * v[b].astype(F32) for b in range(a + 1)], axis=0)
            high = prod.astype(BF16)
            low = (prod - high.astype(F32)).astype(BF16)
            sums = mm(high, bd[...]) + mm(low, bd[...])
            base = a * (a + 1) // 2
            grads = [sums[b * 128 : (b + 1) * 128] for b in range(a + 1)]
            inner = functools.reduce(jnp.add, [wts[base + b] * grads[b] for b in range(a + 1)])
            dq = jnp.zeros((128, 256), F32)
            for b in range(a + 1):
                w = wts[base + b]
                sgrad = (w * (grads[b] - inner) * 0.125).astype(BF16).astype(F32)
                dq = dq + sgrad * k[b].astype(F32)
                dk_b = sgrad * q[a].astype(F32)
                dv_b = w.astype(BF16).astype(F32) * out_grad
                if a == KW - 1:
                    dkv[0, b] = dk_b
                    dkv[1, b] = dv_b
                else:
                    dkv[0, b] = dkv[0, b] + dk_b
                    dkv[1, b] = dkv[1, b] + dv_b
            dk = dkv[0, a]
            dv = dkv[1, a]
        big[...] = (
            mm_t(dq.astype(BF16), wqkv[0]) + mm_t(dk.astype(BF16), wqkv[1]) + mm_t(dv.astype(BF16), wqkv[2])
        )

        def rows_of(rb, c):
            rows = pl.ds(pl.multiple_of(rb * RB, RB), RB)
            val = s_in[a, rows, :]
            cot = big[rows, :] * ga[...]
            scale = lax.rsqrt(jnp.mean(val * val, axis=1, keepdims=True) + EPS)
            along = jnp.mean(cot * val, axis=1, keepdims=True) * (scale * scale * scale)
            midsum[rows, :] = midsum[rows, :] + cot * scale - val * along
            return c

        lax.fori_loop(0, 128 // RB, rows_of, 0)

    e_s[...] = midsum[:, other].astype(BF16)
    e1 = remote(e_s, e_r, e_ss.at[0], e_rs.at[0], to_p)
    e1.start()
    e1.wait_recv()
    e_2[chip, core] = (midsum[:, mine] + e_r[...].astype(F32)).astype(BF16)
    e2x = remote(e_2.at[chip, core], e_2.at[chip, core], e_ss.at[1], e_rs.at[1], to_x)
    e2p = remote(e_2.at[chip, core], e_2.at[chip, core], e_ss.at[2], e_rs.at[2], to_p)
    e2x.start()
    e2p.start()
    landed(e_2.at[1 - chip, core], e_rs.at[1])
    relay(e_2.at[1 - chip, core], e_ss.at[3], e_rs.at[3])
    landed(e_2.at[chip, 1 - core], e_rs.at[2])
    landed(e_2.at[1 - chip, 1 - core], e_rs.at[3])
    for h in range(2):
        cg[:, h * 512 : (h + 1) * 512] = (e_2[0, h].astype(F32) + e_2[1, h].astype(F32)).astype(BF16)

    for j in range(8):
        block = cg[:, j * 128 : (j + 1) * 128].astype(F32).T.astype(BF16)
        step = min(cw, 128)
        for m in range(128 // step):
            col = j * 128 + m * step
            owner = col // cw
            yy, zz, xx = owner % ys, (owner // ys) % zs, owner // (ys * zs)
            at = (xx * zh_n + zz // zb_n) * cw + col % cw
            tsend[(zz % zb_n) * ys + yy, at : at + step, :] = block[m * step : (m + 1) * step]
    tails = []
    for n, peer in enumerate(pos_peers):
        copy = remote(tsend.at[peer], trecv.at[pos], t_ss.at[n], t_rs.at[pos], {"seq": seq_of(peer, sg)})
        copy.start()
        tails.append(copy)
    trecv[pos] = tsend[pos]

    wproj_rows = 256
    for n in range(1024 // wproj_rows):
        cols = slice(n * wproj_rows, (n + 1) * wproj_rows)
        normed[0, :, cols] = mm_t(cg[...], wproj[cols, :]).astype(BF16)
    o_hid = pltpu.make_async_copy(normed.at[0], ghid_o, lsem.at[11])
    o_hid.start()

    part[...] = mm(trecv[pos], hg[pos])
    for peer in pos_peers:
        landed(hg.at[peer], hid_rs.at[peer]) if zb_n == 1 else None
    if zb_n > 1:
        for n in range(1, npos):
            slot = lax.rem(pos + n, npos)

            @pl.when(slot != pos_z)
            def _():
                landed(hg.at[slot], hid_rs.at[slot])

    for peer in pos_peers:
        landed(trecv.at[peer], t_rs.at[peer])
        part[...] = part[...] + mm(trecv[peer], hg[peer])
    for n in range(nsg):
        psend[n] = part[n * cw : (n + 1) * cw, :].astype(BF16)
    for n, peer in enumerate(sg_peers):
        copy = remote(psend.at[peer], precv.at[sg], p_ss.at[n], p_rs.at[sg], {"seq": seq_of(pos, peer)})
        copy.start()
        tails.append(copy)
    precv[sg] = psend[sg]
    for peer in sg_peers:
        landed(precv.at[peer], p_rs.at[peer])
    gproj_o[...] = functools.reduce(jnp.add, [precv[n].astype(F32) for n in range(nsg)])

    o_hid.wait()
    for copy in (c1, w_p, w_x, c2x, c2p, e1, e2x, e2p, *looks, *hids, *relays, *stats, *tails):
        copy.wait_send()
    for i in range(KW):
        remote(b_s.at[i], b_r.at[i], b_ss.at[i, 0], b_rs.at[i, 0], to_p).wait_send()
        remote(b_s2.at[i], b_r2.at[i], b_ss.at[i, 1], b_rs.at[i, 1], to_x).wait_send()


def body(hidden, w_proj, codes, embed_table, w_qkv, w_out, head_table, gain_attn, gain_head):
    seq_size = lax.axis_size("seq")
    xs, zs, ys = LAYOUT[seq_size]
    npos = min(2, zs) * ys
    nsg = seq_size // npos
    cw = 1024 // seq_size
    vm, dma = pltpu.VMEM, pltpu.SemaphoreType.DMA
    scratch = [
        vm((npos, 128, 1024), BF16), vm((1024, 1024), BF16), vm((KW, 128), jnp.int32),
        vm((3, 2048, 256), BF16), vm((3, 1024, 256), BF16), vm((TP, 256, 1024), BF16),
        vm((KW, 1024, 512), BF16), vm((1, 1024), F32), vm((1, 1024), F32),
        vm((KW, 128, 128), jnp.int32), vm((TP, 3, 128, 256), BF16),
        vm((128, 512), BF16), vm((128, 512), BF16), vm((2, 2, 128, 512), BF16),
        vm((KW, 128, 1024), F32), vm((KW, 128, 1024), F32), vm((KW, 128, 1024), BF16),
        vm((KW, 128, 256), BF16), vm((KW, 128, 256), BF16), vm((KW, 128, 256), BF16),
        vm((10, 128, 256), F32), vm((TP, KW, 128, 256), BF16), vm((256, 256), BF16),
        vm((128, 1024), F32), vm((KW, 256, 1024), F32), vm((128, 128), F32),
        vm((TP, 24, 128), F32), vm((128, 128), F32), vm((128, 1024), F32),
        vm((KW, 2, 128, 256), BF16), vm((KW, 2, 128, 256), BF16), vm((KW, 128, 256), BF16),
        vm((KW, 128, 256), BF16), vm((KW, 2, 128, 256), F32), vm((2, KW, 128, 256), F32),
        vm((8, 128), F32),
        vm((128, 512), BF16), vm((128, 512), BF16), vm((2, 2, 128, 512), BF16), vm((128, 1024), BF16),
        vm((npos, nsg * cw, 128), BF16), vm((npos, nsg * cw, 128), BF16),
        vm((nsg, cw, 1024), BF16), vm((nsg, cw, 1024), BF16), vm((nsg * cw, 1024), F32),
        dma((16,)), dma((8,)), dma((8,)), dma((3,)), dma((8,)), dma((3, 3)), dma((3, 8)),
        dma((4,)), dma((4,)), dma((KW, 3)), dma((KW, 8)), dma((3,)), dma((4,)),
        dma((KW, 2)), dma((KW, 2)), dma((4,)), dma((4,)), dma((8,)), dma((8,)), dma((8,)), dma((8,)),
    ]
    hbm = pl.BlockSpec(memory_space=pl.ANY)
    vmem = pl.BlockSpec(memory_space=pltpu.VMEM)
    loss, grad_hidden, grad_proj = pl.pallas_call(
        functools.partial(kernel, seq_size),
        out_shape=(
            jax.ShapeDtypeStruct((KW, 128), F32),
            jax.ShapeDtypeStruct((128, 1024), BF16),
            jax.ShapeDtypeStruct((cw, 1024), F32),
        ),
        in_specs=[hbm] * 9,
        out_specs=(vmem, hbm, vmem),
        scratch_shapes=scratch,
        compiler_params=pltpu.CompilerParams(
            collective_id=0, has_side_effects=True, vmem_limit_bytes=60 * 2**20
        ),
        name="depth_window",
    )(
        hidden, w_proj, codes.T, embed_table, jnp.transpose(w_qkv, (1, 0, 2)), w_out, head_table,
        gain_attn.reshape(1, -1), gain_head.reshape(1, -1),
    )
    return loss.T, grad_hidden, grad_proj.T


def solution(mesh):
    return jax.shard_map(
        body,
        mesh=mesh,
        in_specs=(
            P("seq", "tp"),
            P("tp", None),
            P("seq", None),
            P(None, None, "tp"),
            P(None, None, "tp"),
            P("tp", None),
            P(None, None, "tp"),
            P(),
            P(),
        ),
        out_specs=(P("seq", None), P("seq", "tp"), P("tp", "seq")),
        check_vma=False,
    )
```

```python
import functools

import jax
import jax.numpy as jnp
from jax import lax
from jax.experimental import pallas as pl
from jax.experimental.pallas import tpu as pltpu
from jax.sharding import PartitionSpec as P

HEADS = 16
KW = 4
TP = 4
EPS = 1e-06
RB = 32
F32 = jnp.float32
BF16 = jnp.bfloat16
MESH = pl.DeviceIdType.MESH
LAYOUT = {64: (2, 8, 4), 8: (2, 2, 2)}


def mm(a, b):
    return jnp.dot(a, b, preferred_element_type=F32)


def mm_t(a, b):
    return lax.dot_general(a, b, (((1,), (1,)), ((), ())), preferred_element_type=F32)


def remote(src, dst, send, recv, device):
    return pltpu.make_async_remote_copy(
        src_ref=src, dst_ref=dst, send_sem=send, recv_sem=recv, device_id=device, device_id_type=MESH
    )


def kernel(
    seq_size,
    hid_h, wproj_h, codes_h, emb_h, wqkv_h, wo_h, head_h, ga_h, gh_h,
    loss_o, ghid_o, gproj_o,
    hg, wproj, codes, emb, wqkv, wo, head, ga, gh,
    ccol, looked, c_s, c_r, c_2, s_in, s_mid, normed, q, k, v, wts, att, bd,
    big, g1, g2, ep, r_in, r_mid, st_c, st, sc, midsum, b_s, b_r, b_s2, b_r2, ag, dkv, dqkv,
    e_s, e_r, e_2, cg, tsend, trecv, psend, precv, part,
    lsem, hid_ss, hid_rs, wo_ss, wo_rs, lk_ss, lk_rs, c_ss, c_rs, att_ss, att_rs,
    st_ss, st_rs, b_ss, b_rs, e_ss, e_rs, t_ss, t_rs, p_ss, p_rs,
):
    xs, zs, ys = LAYOUT[seq_size]
    zb_n = min(2, zs)
    zh_n = zs // zb_n
    npos, nsg = zb_n * ys, xs * zh_n
    cw = 1024 // seq_size
    total = float(128 * seq_size * KW)

    r = lax.axis_index("tp")
    s = lax.axis_index("seq")
    core = r % 2
    chip = r // 2
    p = chip * 2 + (1 - core)
    x = (1 - chip) * 2 + core
    d = (1 - chip) * 2 + (1 - core)
    y = s % ys
    z = (s // ys) % zs
    xh = s // (ys * zs)
    pos = (z % zb_n) * ys + y
    sg = xh * zh_n + z // zb_n
    to_p, to_x, to_d = {"tp": p}, {"tp": x}, {"tp": d}
    flip = {"seq": (xs - 1 - xh) * (ys * zs) + z * ys + y, "tp": x}

    def seq_of(position, supergroup):
        yy, zb = position % ys, position // ys
        zh, xx = supergroup % zh_n, supergroup // zh_n
        return xx * (ys * zs) + (zh * zb_n + zb) * ys + yy

    pos_peers = [lax.rem(pos + i, npos) for i in range(1, npos)]
    sg_peers = [lax.rem(sg + i, nsg) for i in range(1, nsg)]

    def load(src, dst, i):
        copy = pltpu.make_async_copy(src, dst, lsem.at[i])
        copy.start()
        return copy

    l_hid = load(hid_h, hg.at[pos], 0)
    l_wproj = load(wproj_h, wproj, 1)
    l_codes = load(codes_h, codes, 2)
    l_emb = [load(emb_h.at[i], emb.at[i], 3 + i) for i in range(3)]
    l_ga = load(ga_h, ga, 6)
    l_gh = load(gh_h, gh, 7)
    l_qkv = load(wqkv_h, wqkv, 8)
    l_wo = load(wo_h, wo.at[r], 9)
    l_head = load(head_h, head, 10)

    barrier = pltpu.get_barrier_semaphore()
    peers = [to_p, to_x, to_d, flip]
    peers += [{"seq": seq_of(i, sg)} for i in pos_peers]
    peers += [{"seq": seq_of(i, sg), "tp": p} for i in pos_peers]
    peers += [{"seq": seq_of(pos, i)} for i in sg_peers]
    for peer in peers:
        pl.semaphore_signal(barrier, inc=1, device_id=peer, device_id_type=MESH)

    lane = lax.broadcasted_iota(jnp.int32, (128, 128), 1)
    bd[...] = (
        lax.broadcasted_iota(jnp.int32, (256, 256), 0) // 64
        == lax.broadcasted_iota(jnp.int32, (256, 256), 1) // 64
    ).astype(F32).astype(BF16)
    l_codes.wait()
    st_c[...] = jnp.zeros_like(st_c)
    st_c[0:KW, :] = codes[...].astype(F32)
    code_cols = st_c[...].T
    for i in range(KW):
        ccol[i] = jnp.broadcast_to(code_cols[:, i : i + 1], (128, 128)).astype(jnp.int32)
    l_hid.wait()
    l_wproj.wait()
    mine = pl.ds(pl.multiple_of(core * 512, 512), 512)
    other = pl.ds(pl.multiple_of((1 - core) * 512, 512), 512)
    c_s[...] = mm(hg[pos], wproj[:, other]).astype(BF16)
    big[:, 0:512] = mm(hg[pos], wproj[:, mine])
    for i in range(KW - 1):
        l_emb[i].wait()
        code = ccol[i]
        hot = jnp.concatenate(
            [(code == lane + 128 * g).astype(F32).astype(BF16) for g in range(16)], axis=1
        )
        looked[r, i] = mm(hot, emb[i]).astype(BF16)

    pl.semaphore_wait(barrier, len(peers))

    relays = []

    def send(src, dst, ss, rs, to):
        copy = remote(src, dst, ss, rs, to)
        copy.start()
        relays.append(copy)

    def relay(buf, ss, rs):
        send(buf, buf, ss, rs, to_p)

    def landed(buf, recv):
        remote(buf, buf, lsem.at[15], recv, to_p).wait_recv()

    def look(i, n):
        send(looked.at[r, i], looked.at[r, i], lk_ss.at[i, n], lk_rs.at[i, r], (to_x, to_p)[n])

    c1 = remote(c_s, c_r, c_ss.at[0], c_rs.at[0], to_p)
    c1.start()
    look(0, 0)
    c1.wait_recv()
    c_2[chip, core] = (big[:, 0:512] + c_r[...].astype(F32)).astype(BF16)
    send(c_2.at[chip, core], c_2.at[chip, core], c_ss.at[1], c_rs.at[1], to_x)
    send(c_2.at[chip, core], c_2.at[chip, core], c_ss.at[2], c_rs.at[2], to_p)
    look(1, 0)
    look(2, 0)
    look(0, 1)
    look(1, 1)
    look(2, 1)

    send(wo_h, wo.at[r], wo_ss.at[1], wo_rs.at[r], flip)
    send(wo_h, wo.at[r], wo_ss.at[0], wo_rs.at[r], to_p)

    for n in range(1, ys):
        py = lax.rem(y + n, ys)
        send(hid_h, hg.at[pos], hid_ss.at[n - 1], hid_rs.at[pos], {"seq": seq_of((z % zb_n) * ys + py, sg)})
    pos_z = (1 - z % zb_n) * ys + y
    send(hid_h, hg.at[pos], hid_ss.at[3], hid_rs.at[pos], {"seq": seq_of(pos_z, sg)})

    def vocab_hit(i):
        code = ccol[i]
        return jnp.concatenate([code == lane + (128 * g + r * 512) for g in range(4)], axis=1)

    def hot_product(i):
        g2[i] = mm_t(vocab_hit(i).astype(F32).astype(BF16), head[i]).astype(BF16)

    landed(looked.at[x, 0], lk_rs.at[0, x])
    relay(looked.at[x, 0], lk_ss.at[0, 2], lk_rs.at[0, x + 4])
    l_head.wait()
    hot_product(0)
    landed(c_2.at[1 - chip, core], c_rs.at[1])
    relay(c_2.at[1 - chip, core], c_ss.at[3], c_rs.at[3])
    hot_product(1)
    l_ga.wait()
    landed(c_2.at[chip, 1 - core], c_rs.at[2])
    landed(c_2.at[1 - chip, 1 - core], c_rs.at[3])

    def stream_rows(i):
        for rb in range(128 // RB):
            rows = slice(rb * RB, (rb + 1) * RB)
            ctx = jnp.concatenate(
                [c_2[0, h, rows, :].astype(F32) + c_2[1, h, rows, :].astype(F32) for h in range(2)], axis=1
            )
            if i > 0:
                ctx = ctx + jnp.concatenate([looked[j, i - 1, rows, :].astype(F32) for j in range(TP)], axis=1)
            s_in[i, rows, :] = ctx
            scale = lax.rsqrt(jnp.mean(ctx * ctx, axis=1, keepdims=True) + EPS)
            r_in[i, rows, :] = jnp.broadcast_to(scale, (RB, 128))
            normed[i, rows, :] = (ctx * scale * ga[...]).astype(BF16)

    def project(i):
        for n, dst in enumerate((q, k, v)):
            dst[i] = mm(normed[i], wqkv[n]).astype(BF16)

    def attend(a):
        probe = [q[a].astype(F32) * k[b].astype(F32) for b in range(a + 1)]
        if a == 0:
            att[r, 0] = v[0]
        else:
            prod = jnp.concatenate(probe, axis=0)
            high = prod.astype(BF16)
            low = (prod - high.astype(F32)).astype(BF16)
            sums = (mm(high, bd[...]) + mm(low, bd[...])) * 0.125
            rows = [sums[b * 128 : (b + 1) * 128] for b in range(a + 1)]
            top = functools.reduce(jnp.maximum, rows)
            rows = [jnp.exp(row - top) for row in rows]
            inv = 1.0 / functools.reduce(jnp.add, rows)
            out = jnp.zeros((128, 256), F32)
            for b in range(a + 1):
                w = rows[b] * inv
                wts[a * (a + 1) // 2 + b] = w
                out = out + w.astype(BF16).astype(F32) * v[b].astype(F32)
            att[r, a] = out.astype(BF16)
        for n, to in enumerate((to_x, to_p)):
            send(att.at[r, a], att.at[r, a], att_ss.at[a, n], att_rs.at[a, r], to)

    for i in range(KW):
        if i > 0:
            if i > 1:
                landed(looked.at[x, i - 1], lk_rs.at[i - 1, x])
                relay(looked.at[x, i - 1], lk_ss.at[i - 1, 2], lk_rs.at[i - 1, x + 4])
                hot_product(i)
            landed(looked.at[p, i - 1], lk_rs.at[i - 1, p])
            landed(looked.at[d, i - 1], lk_rs.at[i - 1, d + 4])
        stream_rows(i)
        if i == 0:
            l_qkv.wait()
        project(i)
        attend(i)

    landed(hg.at[pos_z], hid_rs.at[pos_z])
    for n in range(1, ys):
        py = lax.rem(y + n, ys)
        send(hg.at[pos_z], hg.at[pos_z], hid_ss.at[3 + n], hid_rs.at[pos_z], {"seq": seq_of((z % zb_n) * ys + py, sg)})
    landed(wo.at[x], wo_rs.at[x])
    relay(wo.at[x], wo_ss.at[2], wo_rs.at[x + 4])
    l_wo.wait()
    landed(wo.at[p], wo_rs.at[p])
    l_gh.wait()
    st_c[...] = jnp.zeros_like(st_c)
    midsum[...] = jnp.zeros_like(midsum)

    def forward(i, carry):
        landed(att.at[x, i], att_rs.at[i, x])
        copy = remote(att.at[x, i], att.at[x, i], att_ss.at[i, 2], att_rs.at[i, x + 4], to_p)
        copy.start()
        acc = s_in[i] + mm(att[r, i], wo[r])
        landed(att.at[p, i], att_rs.at[i, p])
        big[...] = acc + mm(att[p, i], wo[p]) + mm(att[x, i], wo[x])

        @pl.when(i == 0)
        def _():
            landed(wo.at[d], wo_rs.at[d + 4])

        landed(att.at[d, i], att_rs.at[i, d + 4])
        s_mid[i] = big[...] + mm(att[d, i], wo[d])

        for rb in range(128 // RB):
            rows = slice(rb * RB, (rb + 1) * RB)
            val = s_mid[i, rows, :]
            scale = lax.rsqrt(jnp.mean(val * val, axis=1, keepdims=True) + EPS)
            r_mid[i, rows, :] = jnp.broadcast_to(scale, (RB, 128))
            normed[i, rows, :] = (val * scale * gh[...]).astype(BF16)
        logits = mm(normed[i], head[i])
        hit = vocab_hit(i)
        top = jnp.max(logits, axis=1, keepdims=True)
        grown = jnp.exp(logits - top)
        total_exp = jnp.sum(grown, axis=1, keepdims=True)
        target = jnp.sum(jnp.where(hit, logits, 0.0), axis=1, keepdims=True)
        st_c[...] = jnp.where(
            lane == i, top, jnp.where(lane == i + 8, total_exp, jnp.where(lane == i + 16, target, st_c[...]))
        )
        ep[i] = jnp.where(hit, 0.0, grown).astype(BF16)
        copy.wait_send()
        return carry

    lax.fori_loop(0, KW, forward, 0)

    st[r] = st_c[...].T[0:24, :]
    stats = []
    for n, to in enumerate((to_p, to_x, to_d)):
        copy = remote(st.at[r], st.at[r], st_ss.at[n], st_rs.at[r], to)
        copy.start()
        stats.append(copy)
    for i in range(KW):
        g1[i] = mm_t(ep[i], head[i])
    for slot in (p, x, d):
        landed(st.at[slot], st_rs.at[slot])
    tops = [st[j, 0:8, :] for j in range(TP)]
    top = functools.reduce(jnp.maximum, tops)
    exp_total = functools.reduce(jnp.add, [st[j, 8:16, :] * jnp.exp(tops[j] - top) for j in range(TP)])
    target = functools.reduce(jnp.add, [st[j, 16:24, :] for j in range(TP)])
    log_total = top + jnp.log(exp_total)
    loss_o[...] = (log_total - target)[0:KW, :]
    sc[...] = jnp.zeros_like(sc)
    sc[0:8, :] = jnp.exp(st[r, 0:8, :] - log_total) * (1.0 / total)
    sc[8:16, :] = (jnp.exp(target - log_total) - 1.0) * (1.0 / total)
    sc[...] = sc[...].T

    def send_on(i):
        landed(b_r.at[i], b_rs.at[i, 0])
        b_s2[i] = (ag[i, 1] + b_r[i, 1].astype(F32)).astype(BF16)
        remote(b_s2.at[i], b_r2.at[i], b_ss.at[i, 1], b_rs.at[i, 1], to_x).start()

    def head_back(n, carry):
        i = KW - 1 - n

        for rb in range(128 // RB):
            rows = slice(rb * RB, (rb + 1) * RB)
            ln = lax.broadcasted_iota(jnp.int32, (RB, 128), 1)
            both = sc[rows, :]
            grow = jnp.sum(jnp.where(ln == i, both, 0.0), axis=1, keepdims=True)
            hot = jnp.sum(jnp.where(ln == i + 8, both, 0.0), axis=1, keepdims=True)
            val = s_mid[i, rows, :]
            cot = (grow * g1[i, rows, :] + hot * g2[i, rows, :].astype(F32)) * gh[...]
            scale = r_mid[i, rows, 0:1]
            along = jnp.mean(cot * val, axis=1, keepdims=True) * (scale * scale * scale)
            back = cot * scale - val * along
            midsum[rows, :] = midsum[rows, :] + back
            normed[i, rows, :] = back.astype(BF16)

        low = normed[i]
        b_s[i, 0] = mm_t(low, wo[p]).astype(BF16)
        b_s[i, 1] = mm_t(low, wo[d]).astype(BF16)
        remote(b_s.at[i], b_r.at[i], b_ss.at[i, 0], b_rs.at[i, 0], to_p).start()
        ag[i, 1] = mm_t(low, wo[x])
        ag[i, 0] = mm_t(low, wo[r])

        @pl.when(n > 0)
        def _():
            send_on(i + 1)

        return carry

    lax.fori_loop(0, KW, head_back, 0)
    send_on(0)

    for a in range(KW - 1, -1, -1):
        landed(b_r2.at[a], b_rs.at[a, 1])
        out_grad = (ag[a, 0] + b_r[a, 0].astype(F32) + b_r2[a].astype(F32)).astype(BF16).astype(F32)
        if a == 0:
            dq = jnp.zeros((128, 256), F32)
            dk = dkv[0, 0]
            dv = dkv[1, 0] + out_grad
        else:
            prod = jnp.concatenate([out_grad * v[b].astype(F32) for b in range(a + 1)], axis=0)
            high = prod.astype(BF16)
            low = (prod - high.astype(F32)).astype(BF16)
            sums = mm(high, bd[...]) + mm(low, bd[...])
            base = a * (a + 1) // 2
            grads = [sums[b * 128 : (b + 1) * 128] for b in range(a + 1)]
            inner = functools.reduce(jnp.add, [wts[base + b] * grads[b] for b in range(a + 1)])
            dq = jnp.zeros((128, 256), F32)
            for b in range(a + 1):
                w = wts[base + b]
                sgrad = (w * (grads[b] - inner) * 0.125).astype(BF16).astype(F32)
                dq = dq + sgrad * k[b].astype(F32)
                dk_b = sgrad * q[a].astype(F32)
                dv_b = w.astype(BF16).astype(F32) * out_grad
                if a == KW - 1:
                    dkv[0, b] = dk_b
                    dkv[1, b] = dv_b
                else:
                    dkv[0, b] = dkv[0, b] + dk_b
                    dkv[1, b] = dkv[1, b] + dv_b
            dk = dkv[0, a]
            dv = dkv[1, a]
        big[...] = (
            mm_t(dq.astype(BF16), wqkv[0]) + mm_t(dk.astype(BF16), wqkv[1]) + mm_t(dv.astype(BF16), wqkv[2])
        )

        for rb in range(128 // RB):
            rows = slice(rb * RB, (rb + 1) * RB)
            val = s_in[a, rows, :]
            cot = big[rows, :] * ga[...]
            scale = r_in[a, rows, 0:1]
            along = jnp.mean(cot * val, axis=1, keepdims=True) * (scale * scale * scale)
            midsum[rows, :] = midsum[rows, :] + cot * scale - val * along

    e_s[...] = midsum[:, other].astype(BF16)
    e1 = remote(e_s, e_r, e_ss.at[0], e_rs.at[0], to_p)
    e1.start()
    e1.wait_recv()
    e_2[chip, core] = (midsum[:, mine] + e_r[...].astype(F32)).astype(BF16)
    e2x = remote(e_2.at[chip, core], e_2.at[chip, core], e_ss.at[1], e_rs.at[1], to_x)
    e2p = remote(e_2.at[chip, core], e_2.at[chip, core], e_ss.at[2], e_rs.at[2], to_p)
    e2x.start()
    e2p.start()
    landed(e_2.at[1 - chip, core], e_rs.at[1])
    relay(e_2.at[1 - chip, core], e_ss.at[3], e_rs.at[3])

    cg[:, mine] = (e_2[0, core].astype(F32) + e_2[1, core].astype(F32)).astype(BF16)
    for j in range(4):
        block = (
            e_2[0, core, :, j * 128 : (j + 1) * 128].astype(F32) + e_2[1, core, :, j * 128 : (j + 1) * 128].astype(F32)
        ).T.astype(BF16)
        for m in range(128 // cw):
            owner = j * (128 // cw) + m
            yy, zz = owner % ys, owner // ys
            at = (zz // zb_n) * cw
            tsend[(zz % zb_n) * ys + yy, at : at + cw, :] = block[m * cw : (m + 1) * cw]
    for n, peer in enumerate(pos_peers):
        for m, to in enumerate((r, p)):
            send(tsend.at[peer], trecv.at[pos, core], t_ss.at[n, m], t_rs.at[pos, core], {"seq": seq_of(peer, sg), "tp": to})
    send(tsend.at[pos], trecv.at[pos, core], t_ss.at[7, 0], t_rs.at[pos, core], to_p)
    trecv[pos, core] = tsend[pos]

    landed(e_2.at[chip, 1 - core], e_rs.at[2])
    landed(e_2.at[1 - chip, 1 - core], e_rs.at[3])
    cg[:, other] = (e_2[0, 1 - core].astype(F32) + e_2[1, 1 - core].astype(F32)).astype(BF16)
    for n in range(4):
        cols = slice(n * 256, (n + 1) * 256)
        ghid_o[:, cols] = mm_t(cg[...], wproj[cols, :]).astype(BF16)

    for n in range(1, npos):
        slot = lax.rem(pos + n, npos)

        @pl.when(slot != pos_z)
        def _():
            landed(hg.at[slot], hid_rs.at[slot])

    landed(trecv.at[pos, 1 - core], t_rs.at[pos, 1 - core])
    part[...] = mm(trecv[pos].reshape(nsg * cw, 128), hg[pos])
    for peer in pos_peers:
        landed(trecv.at[peer, core], t_rs.at[peer, core])
        landed(trecv.at[peer, 1 - core], t_rs.at[peer, 1 - core])
        part[...] = part[...] + mm(trecv[peer].reshape(nsg * cw, 128), hg[peer])
    for n in range(nsg):
        psend[n] = part[n * cw : (n + 1) * cw, :].astype(BF16)
    for n, peer in enumerate(sg_peers):
        send(psend.at[peer], precv.at[sg], p_ss.at[n], p_rs.at[sg], {"seq": seq_of(pos, peer)})
    precv[sg] = psend[sg]
    for peer in sg_peers:
        landed(precv.at[peer], p_rs.at[peer])
    gproj_o[...] = functools.reduce(jnp.add, [precv[n].astype(F32) for n in range(nsg)])

    for copy in (c1, e1, e2x, e2p, *relays, *stats):
        copy.wait_send()
    for i in range(KW):
        remote(b_s.at[i], b_r.at[i], b_ss.at[i, 0], b_rs.at[i, 0], to_p).wait_send()
        remote(b_s2.at[i], b_r2.at[i], b_ss.at[i, 1], b_rs.at[i, 1], to_x).wait_send()


def hand_out(loss_i, ghid_i, gproj_i, loss_o, ghid_o, gproj_o):
    loss_o[...] = loss_i[...]
    ghid_o[...] = ghid_i[...]
    gproj_o[...] = gproj_i[...]


def body(hidden, w_proj, codes, embed_table, w_qkv, w_out, head_table, gain_attn, gain_head):
    seq_size = lax.axis_size("seq")
    xs, zs, ys = LAYOUT[seq_size]
    npos = min(2, zs) * ys
    nsg = seq_size // npos
    cw = 1024 // seq_size
    vm, dma = pltpu.VMEM, pltpu.SemaphoreType.DMA
    scratch = [
        vm((npos, 128, 1024), BF16), vm((1024, 1024), BF16), vm((KW, 128), jnp.int32),
        vm((3, 2048, 256), BF16), vm((3, 1024, 256), BF16), vm((TP, 256, 1024), BF16),
        vm((KW, 1024, 512), BF16), vm((1, 1024), F32), vm((1, 1024), F32),
        vm((KW, 128, 128), jnp.int32), vm((TP, 3, 128, 256), BF16),
        vm((128, 512), BF16), vm((128, 512), BF16), vm((2, 2, 128, 512), BF16),
        vm((KW, 128, 1024), F32), vm((KW, 128, 1024), F32), vm((KW, 128, 1024), BF16),
        vm((KW, 128, 256), BF16), vm((KW, 128, 256), BF16), vm((KW, 128, 256), BF16),
        vm((10, 128, 256), F32), vm((TP, KW, 128, 256), BF16), vm((256, 256), BF16),
        vm((128, 1024), F32), vm((KW, 128, 1024), F32), vm((KW, 128, 1024), BF16),
        vm((KW, 128, 512), BF16), vm((KW, 128, 128), F32), vm((KW, 128, 128), F32), vm((128, 128), F32),
        vm((TP, 24, 128), F32), vm((128, 128), F32), vm((128, 1024), F32),
        vm((KW, 2, 128, 256), BF16), vm((KW, 2, 128, 256), BF16), vm((KW, 128, 256), BF16),
        vm((KW, 128, 256), BF16), vm((KW, 2, 128, 256), F32), vm((2, KW, 128, 256), F32),
        vm((8, 128), F32),
        vm((128, 512), BF16), vm((128, 512), BF16), vm((2, 2, 128, 512), BF16), vm((128, 1024), BF16),
        vm((npos, nsg * cw // 2, 128), BF16), vm((npos, 2, nsg * cw // 2, 128), BF16),
        vm((nsg, cw, 1024), BF16), vm((nsg, cw, 1024), BF16), vm((nsg * cw, 1024), F32),
        dma((16,)), dma((8,)), dma((8,)), dma((3,)), dma((8,)), dma((3, 3)), dma((3, 8)),
        dma((4,)), dma((4,)), dma((KW, 3)), dma((KW, 8)), dma((3,)), dma((4,)),
        dma((KW, 2)), dma((KW, 2)), dma((4,)), dma((4,)), dma((8, 2)), dma((8, 2)), dma((8,)), dma((8,)),
    ]
    out_shape = (
        jax.ShapeDtypeStruct((KW, 128), F32),
        jax.ShapeDtypeStruct((128, 1024), BF16),
        jax.ShapeDtypeStruct((cw, 1024), F32),
    )
    hbm = pl.BlockSpec(memory_space=pl.ANY)
    vmem = pl.BlockSpec(memory_space=pltpu.VMEM)
    made = pl.pallas_call(
        functools.partial(kernel, seq_size),
        out_shape=out_shape,
        in_specs=[hbm] * 9,
        out_specs=(vmem, vmem, vmem),
        scratch_shapes=scratch,
        compiler_params=pltpu.CompilerParams(
            collective_id=0, has_side_effects=True, vmem_limit_bytes=60 * 2**20
        ),
        name="depth_window",
    )(
        hidden, w_proj, codes.T, embed_table, jnp.transpose(w_qkv, (1, 0, 2)), w_out, head_table,
        gain_attn.reshape(1, -1), gain_head.reshape(1, -1),
    )
    loss, grad_hidden, grad_proj = pl.pallas_call(
        hand_out, out_shape=out_shape, in_specs=[vmem] * 3, out_specs=(vmem,) * 3, name="hand_out"
    )(*made)
    return loss.T, grad_hidden, grad_proj.T


def solution(mesh):
    return jax.shard_map(
        body,
        mesh=mesh,
        in_specs=(
            P("seq", "tp"),
            P("tp", None),
            P("seq", None),
            P(None, None, "tp"),
            P(None, None, "tp"),
            P("tp", None),
            P(None, None, "tp"),
            P(),
            P(),
        ),
        out_specs=(P("seq", None), P("seq", "tp"), P("tp", "seq")),
        check_vma=False,
    )
```

```python
import functools

import jax
import jax.numpy as jnp
from jax import lax
from jax.experimental import pallas as pl
from jax.experimental.pallas import tpu as pltpu
from jax.sharding import PartitionSpec as P

HEADS = 16
KW = 4
TP = 4
EPS = 1e-06
RB = 32
WCUT = 192
F32 = jnp.float32
BF16 = jnp.bfloat16
MESH = pl.DeviceIdType.MESH
LAYOUT = {64: (2, 8, 4), 8: (2, 2, 2)}


def mm(a, b):
    return jnp.dot(a, b, preferred_element_type=F32)


def mm_t(a, b):
    return lax.dot_general(a, b, (((1,), (1,)), ((), ())), preferred_element_type=F32)


def remote(src, dst, send, recv, device):
    return pltpu.make_async_remote_copy(
        src_ref=src, dst_ref=dst, send_sem=send, recv_sem=recv, device_id=device, device_id_type=MESH
    )


def kernel(
    seq_size,
    hid_h, wproj_h, codes_h, emb_h, wqkv_h, wo_h, head_h, ga_h, gh_h,
    loss_o, ghid_o, gproj_o,
    hg, wproj, codes, emb, wqkv, wo, head, ga, gh,
    ccol, looked, c_s, c_r, c_2, s_in, s_mid, normed, q, k, v, wts, att, bd,
    big, g1, g2, ep, r_in, r_mid, st_c, st, sc, midsum, b_s, b_r, b_s2, b_r2, ag, dkv, dqkv,
    e_s, e_r, e_2, cg, tsend, trecv, psend, precv, part,
    lsem, hid_ss, hid_rs, wo_ss, wo_rs, wo_q, lk_ss, lk_rs, c_ss, c_rs, att_ss, att_rs,
    st_ss, st_rs, b_ss, b_rs, e_ss, e_rs, t_ss, t_rs, p_ss, p_rs,
):
    xs, zs, ys = LAYOUT[seq_size]
    zb_n = min(2, zs)
    zh_n = zs // zb_n
    npos, nsg = zb_n * ys, xs * zh_n
    cw = 1024 // seq_size
    total = float(128 * seq_size * KW)

    r = lax.axis_index("tp")
    s = lax.axis_index("seq")
    core = r % 2
    chip = r // 2
    p = chip * 2 + (1 - core)
    x = (1 - chip) * 2 + core
    d = (1 - chip) * 2 + (1 - core)
    y = s % ys
    z = (s // ys) % zs
    xh = s // (ys * zs)
    pos = (z % zb_n) * ys + y
    sg = xh * zh_n + z // zb_n
    to_p, to_x, to_d = {"tp": p}, {"tp": x}, {"tp": d}
    flip = {"seq": (xs - 1 - xh) * (ys * zs) + z * ys + y, "tp": x}

    def seq_of(position, supergroup):
        yy, zb = position % ys, position // ys
        zh, xx = supergroup % zh_n, supergroup // zh_n
        return xx * (ys * zs) + (zh * zb_n + zb) * ys + yy

    def around(size):
        return sorted(range(size), key=lambda i: -min(i, size - i))

    pos_peers = [
        lax.rem(z + n, 2) * ys + lax.rem(y + m, ys) for m in around(ys) for n in (1, 0) if n or m
    ]
    sg_peers = [
        lax.rem(xh + n, xs) * zh_n + lax.rem(z // zb_n + m, zh_n) for m in around(zh_n) for n in (1, 0) if n or m
    ]

    def load(src, dst, i):
        copy = pltpu.make_async_copy(src, dst, lsem.at[i])
        copy.start()
        return copy

    l_hid = load(hid_h, hg.at[pos], 0)
    l_wproj = load(wproj_h, wproj, 1)
    l_codes = load(codes_h, codes, 2)
    l_emb = [load(emb_h.at[i], emb.at[i], 3 + i) for i in range(3)]
    l_ga = load(ga_h, ga, 6)
    l_gh = load(gh_h, gh, 7)
    l_qkv = load(wqkv_h, wqkv, 8)
    l_wo = load(wo_h, wo.at[r], 9)
    l_head = load(head_h, head, 10)

    barrier = pltpu.get_barrier_semaphore()
    peers = [to_p, to_x, to_d, flip]
    peers += [{"seq": seq_of(i, sg)} for i in pos_peers]
    peers += [{"seq": seq_of(i, sg), "tp": p} for i in pos_peers]
    peers += [{"seq": seq_of(pos, i)} for i in sg_peers]
    for peer in peers:
        pl.semaphore_signal(barrier, inc=1, device_id=peer, device_id_type=MESH)

    lane = lax.broadcasted_iota(jnp.int32, (128, 128), 1)
    bd[...] = (
        lax.broadcasted_iota(jnp.int32, (256, 256), 0) // 64
        == lax.broadcasted_iota(jnp.int32, (256, 256), 1) // 64
    ).astype(F32).astype(BF16)
    l_codes.wait()
    st_c[...] = jnp.zeros_like(st_c)
    st_c[0:KW, :] = codes[...].astype(F32)
    code_cols = st_c[...].T
    for i in range(KW):
        ccol[i] = jnp.broadcast_to(code_cols[:, i : i + 1], (128, 128)).astype(jnp.int32)
    l_hid.wait()
    l_wproj.wait()
    mine = pl.ds(pl.multiple_of(core * 512, 512), 512)
    other = pl.ds(pl.multiple_of((1 - core) * 512, 512), 512)
    c_s[...] = mm(hg[pos], wproj[:, other]).astype(BF16)
    big[:, 0:512] = mm(hg[pos], wproj[:, mine])

    def look_up(i):
        l_emb[i].wait()
        code = ccol[i]
        hot = jnp.concatenate(
            [(code == lane + 128 * g).astype(F32).astype(BF16) for g in range(16)], axis=1
        )
        looked[r, i] = mm(hot, emb[i]).astype(BF16)

    look_up(0)

    pl.semaphore_wait(barrier, len(peers))

    relays = []

    def send(src, dst, ss, rs, to):
        copy = remote(src, dst, ss, rs, to)
        copy.start()
        relays.append(copy)

    def relay(buf, ss, rs):
        send(buf, buf, ss, rs, to_p)

    def landed(buf, recv):
        remote(buf, buf, lsem.at[15], recv, to_p).wait_recv()

    def look(i, n):
        send(looked.at[r, i], looked.at[r, i], lk_ss.at[i, n], lk_rs.at[i, r], (to_x, to_p)[n])

    send(wo_h.at[0:WCUT], wo.at[r, 0:WCUT], wo_ss.at[1], wo_rs.at[r], flip)
    c1 = remote(c_s, c_r, c_ss.at[0], c_rs.at[0], to_p)
    c1.start()
    look(0, 0)
    look_up(1)
    c1.wait_recv()
    c_2[chip, core] = (big[:, 0:512] + c_r[...].astype(F32)).astype(BF16)
    send(c_2.at[chip, core], c_2.at[chip, core], c_ss.at[1], c_rs.at[1], to_x)
    send(c_2.at[chip, core], c_2.at[chip, core], c_ss.at[2], c_rs.at[2], to_p)
    look(1, 0)
    look(0, 1)
    look(1, 1)
    look_up(2)
    look(2, 0)
    look(2, 1)
    send(wo_h.at[WCUT:256], wo.at[r, WCUT:256], wo_ss.at[3], wo_q.at[0], to_x)
    send(wo_h, wo.at[r], wo_ss.at[0], wo_rs.at[r], to_p)

    for n in range(1, ys):
        py = lax.rem(y + n, ys)
        send(hid_h, hg.at[pos], hid_ss.at[n - 1], hid_rs.at[pos], {"seq": seq_of((z % zb_n) * ys + py, sg)})
    pos_z = (1 - z % zb_n) * ys + y
    send(hid_h, hg.at[pos], hid_ss.at[3], hid_rs.at[pos], {"seq": seq_of(pos_z, sg)})

    def vocab_hit(i):
        code = ccol[i]
        return jnp.concatenate([code == lane + (128 * g + r * 512) for g in range(4)], axis=1)

    def hot_product(i):
        g2[i] = mm_t(vocab_hit(i).astype(F32).astype(BF16), head[i]).astype(BF16)

    landed(looked.at[x, 0], lk_rs.at[0, x])
    relay(looked.at[x, 0], lk_ss.at[0, 2], lk_rs.at[0, x + 4])
    l_head.wait()
    hot_product(0)
    landed(c_2.at[1 - chip, core], c_rs.at[1])
    relay(c_2.at[1 - chip, core], c_ss.at[3], c_rs.at[3])
    hot_product(1)
    l_ga.wait()
    landed(c_2.at[chip, 1 - core], c_rs.at[2])
    landed(c_2.at[1 - chip, 1 - core], c_rs.at[3])

    def stream_rows(i):
        for rb in range(128 // RB):
            rows = slice(rb * RB, (rb + 1) * RB)
            ctx = jnp.concatenate(
                [c_2[0, h, rows, :].astype(F32) + c_2[1, h, rows, :].astype(F32) for h in range(2)], axis=1
            )
            if i > 0:
                ctx = ctx + jnp.concatenate([looked[j, i - 1, rows, :].astype(F32) for j in range(TP)], axis=1)
            s_in[i, rows, :] = ctx
            scale = lax.rsqrt(jnp.mean(ctx * ctx, axis=1, keepdims=True) + EPS)
            r_in[i, rows, :] = jnp.broadcast_to(scale, (RB, 128))
            normed[i, rows, :] = (ctx * scale * ga[...]).astype(BF16)

    def project(i):
        for n, dst in enumerate((q, k, v)):
            dst[i] = mm(normed[i], wqkv[n]).astype(BF16)

    def attend(a):
        probe = [q[a].astype(F32) * k[b].astype(F32) for b in range(a + 1)]
        if a == 0:
            att[r, 0] = v[0]
        else:
            prod = jnp.concatenate(probe, axis=0)
            high = prod.astype(BF16)
            low = (prod - high.astype(F32)).astype(BF16)
            sums = (mm(high, bd[...]) + mm(low, bd[...])) * 0.125
            rows = [sums[b * 128 : (b + 1) * 128] for b in range(a + 1)]
            top = functools.reduce(jnp.maximum, rows)
            rows = [jnp.exp(row - top) for row in rows]
            inv = 1.0 / functools.reduce(jnp.add, rows)
            out = jnp.zeros((128, 256), F32)
            for b in range(a + 1):
                w = rows[b] * inv
                wts[a * (a + 1) // 2 + b] = w
                out = out + w.astype(BF16).astype(F32) * v[b].astype(F32)
            att[r, a] = out.astype(BF16)
        for n, to in enumerate((to_x, to_p)):
            send(att.at[r, a], att.at[r, a], att_ss.at[a, n], att_rs.at[a, r], to)

    for i in range(KW):
        if i > 0:
            if i > 1:
                landed(looked.at[x, i - 1], lk_rs.at[i - 1, x])
                relay(looked.at[x, i - 1], lk_ss.at[i - 1, 2], lk_rs.at[i - 1, x + 4])
                hot_product(i)
            landed(looked.at[p, i - 1], lk_rs.at[i - 1, p])
            landed(looked.at[d, i - 1], lk_rs.at[i - 1, d + 4])
        stream_rows(i)
        if i == 0:
            l_qkv.wait()
        project(i)
        attend(i)

    landed(hg.at[pos_z], hid_rs.at[pos_z])
    for n in range(1, ys):
        py = lax.rem(y + n, ys)
        send(hg.at[pos_z], hg.at[pos_z], hid_ss.at[3 + n], hid_rs.at[pos_z], {"seq": seq_of((z % zb_n) * ys + py, sg)})
    l_wo.wait()
    for i in range(KW):
        s_mid[i] = s_in[i] + mm(att[r, i], wo[r])
    landed(wo.at[p], wo_rs.at[p])
    for i in range(KW):
        landed(att.at[p, i], att_rs.at[i, p])
        s_mid[i] = s_mid[i] + mm(att[p, i], wo[p])
    landed(wo.at[x, 0:WCUT], wo_rs.at[x])
    relay(wo.at[x, 0:WCUT], wo_ss.at[2], wo_rs.at[x + 4])
    landed(wo.at[x, WCUT:256], wo_q.at[0])
    relay(wo.at[x, WCUT:256], wo_ss.at[4], wo_q.at[1])
    l_gh.wait()
    midsum[...] = jnp.zeros_like(midsum)

    def norm_mid(i):
        for rb in range(128 // RB):
            rows = slice(rb * RB, (rb + 1) * RB)
            val = s_mid[i, rows, :]
            scale = lax.rsqrt(jnp.mean(val * val, axis=1, keepdims=True) + EPS)
            r_mid[i, rows, :] = jnp.broadcast_to(scale, (RB, 128))
            normed[i, rows, :] = (val * scale * gh[...]).astype(BF16)

    def heads(i):
        logits = mm(normed[i], head[i])
        hit = vocab_hit(i)
        top = jnp.max(logits, axis=1, keepdims=True)
        grown = jnp.exp(logits - top)
        total_exp = jnp.sum(grown, axis=1, keepdims=True)
        target = jnp.sum(jnp.where(hit, logits, 0.0), axis=1, keepdims=True)
        ep[i] = jnp.where(hit, 0.0, grown).astype(BF16)
        return top, total_exp, target

    found = []
    for pair in ((0, 1), (2, 3)):
        for i in pair:
            landed(att.at[x, i], att_rs.at[i, x])
            relay(att.at[x, i], att_ss.at[i, 2], att_rs.at[i, x + 4])
        for i in pair:
            s_mid[i] = s_mid[i] + mm(att[x, i], wo[x])
        if pair[0] == 0:
            landed(wo.at[d, 0:WCUT], wo_rs.at[d + 4])
            landed(wo.at[d, WCUT:256], wo_q.at[1])
        for i in pair:
            landed(att.at[d, i], att_rs.at[i, d + 4])
        for i in pair:
            s_mid[i] = s_mid[i] + mm(att[d, i], wo[d])
        for i in pair:
            norm_mid(i)
        found += [heads(i) for i in pair]
    rows_st = jnp.zeros((128, 128), F32)
    for i in range(KW):
        for n in range(3):
            rows_st = jnp.where(lane == i + 8 * n, found[i][n], rows_st)
    st_c[...] = rows_st
    st[r] = st_c[...].T[0:24, :]
    stats = []
    for n, to in enumerate((to_p, to_x, to_d)):
        copy = remote(st.at[r], st.at[r], st_ss.at[n], st_rs.at[r], to)
        copy.start()
        stats.append(copy)
    for i in range(KW):
        g1[i] = mm_t(ep[i], head[i])
    for slot in (p, x, d):
        landed(st.at[slot], st_rs.at[slot])
    tops = [st[j, 0:8, :] for j in range(TP)]
    top = functools.reduce(jnp.maximum, tops)
    exp_total = functools.reduce(jnp.add, [st[j, 8:16, :] * jnp.exp(tops[j] - top) for j in range(TP)])
    target = functools.reduce(jnp.add, [st[j, 16:24, :] for j in range(TP)])
    log_total = top + jnp.log(exp_total)
    loss_o[...] = (log_total - target)[0:KW, :]
    sc[...] = jnp.zeros_like(sc)
    sc[0:8, :] = jnp.exp(st[r, 0:8, :] - log_total) * (1.0 / total)
    sc[8:16, :] = (jnp.exp(target - log_total) - 1.0) * (1.0 / total)
    sc[...] = sc[...].T

    def send_on(i):
        landed(b_r.at[i], b_rs.at[i, 0])
        b_s2[i] = (ag[i, 1] + b_r[i, 1].astype(F32)).astype(BF16)
        remote(b_s2.at[i], b_r2.at[i], b_ss.at[i, 1], b_rs.at[i, 1], to_x).start()

    def head_back(n, carry):
        i = KW - 1 - n

        for rb in range(128 // RB):
            rows = slice(rb * RB, (rb + 1) * RB)
            ln = lax.broadcasted_iota(jnp.int32, (RB, 128), 1)
            both = sc[rows, :]
            grow = jnp.sum(jnp.where(ln == i, both, 0.0), axis=1, keepdims=True)
            hot = jnp.sum(jnp.where(ln == i + 8, both, 0.0), axis=1, keepdims=True)
            val = s_mid[i, rows, :]
            cot = (grow * g1[i, rows, :] + hot * g2[i, rows, :].astype(F32)) * gh[...]
            scale = r_mid[i, rows, 0:1]
            along = jnp.mean(cot * val, axis=1, keepdims=True) * (scale * scale * scale)
            back = cot * scale - val * along
            midsum[rows, :] = midsum[rows, :] + back
            normed[i, rows, :] = back.astype(BF16)

        low = normed[i]
        b_s[i, 0] = mm_t(low, wo[p]).astype(BF16)
        b_s[i, 1] = mm_t(low, wo[d]).astype(BF16)
        remote(b_s.at[i], b_r.at[i], b_ss.at[i, 0], b_rs.at[i, 0], to_p).start()

        @pl.when(n > 0)
        def _():
            send_on(i + 1)

        ag[i, 1] = mm_t(low, wo[x])
        ag[i, 0] = mm_t(low, wo[r])
        return carry

    lax.fori_loop(0, KW, head_back, 0)
    send_on(0)

    for a in range(KW - 1, -1, -1):
        landed(b_r2.at[a], b_rs.at[a, 1])
        out_grad = (ag[a, 0] + b_r[a, 0].astype(F32) + b_r2[a].astype(F32)).astype(BF16).astype(F32)
        if a == 0:
            dq = jnp.zeros((128, 256), F32)
            dk = dkv[0, 0]
            dv = dkv[1, 0] + out_grad
        else:
            prod = jnp.concatenate([out_grad * v[b].astype(F32) for b in range(a + 1)], axis=0)
            high = prod.astype(BF16)
            low = (prod - high.astype(F32)).astype(BF16)
            sums = mm(high, bd[...]) + mm(low, bd[...])
            base = a * (a + 1) // 2
            grads = [sums[b * 128 : (b + 1) * 128] for b in range(a + 1)]
            inner = functools.reduce(jnp.add, [wts[base + b] * grads[b] for b in range(a + 1)])
            dq = jnp.zeros((128, 256), F32)
            for b in range(a + 1):
                w = wts[base + b]
                sgrad = (w * (grads[b] - inner) * 0.125).astype(BF16).astype(F32)
                dq = dq + sgrad * k[b].astype(F32)
                dk_b = sgrad * q[a].astype(F32)
                dv_b = w.astype(BF16).astype(F32) * out_grad
                if a == KW - 1:
                    dkv[0, b] = dk_b
                    dkv[1, b] = dv_b
                else:
                    dkv[0, b] = dkv[0, b] + dk_b
                    dkv[1, b] = dkv[1, b] + dv_b
            dk = dkv[0, a]
            dv = dkv[1, a]
        big[...] = (
            mm_t(dq.astype(BF16), wqkv[0]) + mm_t(dk.astype(BF16), wqkv[1]) + mm_t(dv.astype(BF16), wqkv[2])
        )

        for rb in range(128 // RB):
            rows = slice(rb * RB, (rb + 1) * RB)
            val = s_in[a, rows, :]
            cot = big[rows, :] * ga[...]
            scale = r_in[a, rows, 0:1]
            along = jnp.mean(cot * val, axis=1, keepdims=True) * (scale * scale * scale)
            midsum[rows, :] = midsum[rows, :] + cot * scale - val * along

    e_s[...] = midsum[:, other].astype(BF16)
    e1 = remote(e_s, e_r, e_ss.at[0], e_rs.at[0], to_p)
    e1.start()
    e1.wait_recv()
    e_2[chip, core] = (midsum[:, mine] + e_r[...].astype(F32)).astype(BF16)
    e2x = remote(e_2.at[chip, core], e_2.at[chip, core], e_ss.at[1], e_rs.at[1], to_x)
    e2p = remote(e_2.at[chip, core], e_2.at[chip, core], e_ss.at[2], e_rs.at[2], to_p)
    e2x.start()
    e2p.start()
    landed(e_2.at[1 - chip, core], e_rs.at[1])
    relay(e_2.at[1 - chip, core], e_ss.at[3], e_rs.at[3])

    cg[:, mine] = (e_2[0, core].astype(F32) + e_2[1, core].astype(F32)).astype(BF16)
    for j in range(4):
        block = (
            e_2[0, core, :, j * 128 : (j + 1) * 128].astype(F32) + e_2[1, core, :, j * 128 : (j + 1) * 128].astype(F32)
        ).T.astype(BF16)
        for m in range(128 // cw):
            owner = j * (128 // cw) + m
            yy, zz = owner % ys, owner // ys
            at = (zz // zb_n) * cw
            tsend[(zz % zb_n) * ys + yy, at : at + cw, :] = block[m * cw : (m + 1) * cw]
    for n, peer in enumerate(pos_peers):
        for m, to in enumerate((r, p)):
            send(tsend.at[peer], trecv.at[pos, core], t_ss.at[n, m], t_rs.at[pos, core], {"seq": seq_of(peer, sg), "tp": to})
    send(tsend.at[pos], trecv.at[pos, core], t_ss.at[7, 0], t_rs.at[pos, core], to_p)
    trecv[pos, core] = tsend[pos]

    landed(e_2.at[chip, 1 - core], e_rs.at[2])
    landed(e_2.at[1 - chip, 1 - core], e_rs.at[3])
    cg[:, other] = (e_2[0, 1 - core].astype(F32) + e_2[1, 1 - core].astype(F32)).astype(BF16)
    for n in range(4):
        cols = slice(n * 256, (n + 1) * 256)
        ghid_o[:, cols] = mm_t(cg[...], wproj[cols, :]).astype(BF16)

    for n in range(1, npos):
        slot = lax.rem(pos + n, npos)

        @pl.when(slot != pos_z)
        def _():
            landed(hg.at[slot], hid_rs.at[slot])

    landed(trecv.at[pos, 1 - core], t_rs.at[pos, 1 - core])
    part[...] = mm(trecv[pos].reshape(nsg * cw, 128), hg[pos])
    for peer in pos_peers:
        landed(trecv.at[peer, core], t_rs.at[peer, core])
        landed(trecv.at[peer, 1 - core], t_rs.at[peer, 1 - core])
        part[...] = part[...] + mm(trecv[peer].reshape(nsg * cw, 128), hg[peer])
    for n in range(nsg):
        psend[n] = part[n * cw : (n + 1) * cw, :].astype(BF16)
    for n, peer in enumerate(sg_peers):
        send(psend.at[peer], precv.at[sg], p_ss.at[n], p_rs.at[sg], {"seq": seq_of(pos, peer)})
    precv[sg] = psend[sg]
    for peer in sg_peers:
        landed(precv.at[peer], p_rs.at[peer])
    gproj_o[...] = functools.reduce(jnp.add, [precv[n].astype(F32) for n in range(nsg)])

    for copy in (c1, e1, e2x, e2p, *relays, *stats):
        copy.wait_send()
    for i in range(KW):
        remote(b_s.at[i], b_r.at[i], b_ss.at[i, 0], b_rs.at[i, 0], to_p).wait_send()
        remote(b_s2.at[i], b_r2.at[i], b_ss.at[i, 1], b_rs.at[i, 1], to_x).wait_send()


def hand_out(loss_i, ghid_i, gproj_i, loss_o, ghid_o, gproj_o):
    loss_o[...] = loss_i[...]
    ghid_o[...] = ghid_i[...]
    gproj_o[...] = gproj_i[...]


def body(hidden, w_proj, codes, embed_table, w_qkv, w_out, head_table, gain_attn, gain_head):
    seq_size = lax.axis_size("seq")
    xs, zs, ys = LAYOUT[seq_size]
    npos = min(2, zs) * ys
    nsg = seq_size // npos
    cw = 1024 // seq_size
    vm, dma = pltpu.VMEM, pltpu.SemaphoreType.DMA
    scratch = [
        vm((npos, 128, 1024), BF16), vm((1024, 1024), BF16), vm((KW, 128), jnp.int32),
        vm((3, 2048, 256), BF16), vm((3, 1024, 256), BF16), vm((TP, 256, 1024), BF16),
        vm((KW, 1024, 512), BF16), vm((1, 1024), F32), vm((1, 1024), F32),
        vm((KW, 128, 128), jnp.int32), vm((TP, 3, 128, 256), BF16),
        vm((128, 512), BF16), vm((128, 512), BF16), vm((2, 2, 128, 512), BF16),
        vm((KW, 128, 1024), F32), vm((KW, 128, 1024), F32), vm((KW, 128, 1024), BF16),
        vm((KW, 128, 256), BF16), vm((KW, 128, 256), BF16), vm((KW, 128, 256), BF16),
        vm((10, 128, 256), F32), vm((TP, KW, 128, 256), BF16), vm((256, 256), BF16),
        vm((128, 1024), F32), vm((KW, 128, 1024), F32), vm((KW, 128, 1024), BF16),
        vm((KW, 128, 512), BF16), vm((KW, 128, 128), F32), vm((KW, 128, 128), F32), vm((128, 128), F32),
        vm((TP, 24, 128), F32), vm((128, 128), F32), vm((128, 1024), F32),
        vm((KW, 2, 128, 256), BF16), vm((KW, 2, 128, 256), BF16), vm((KW, 128, 256), BF16),
        vm((KW, 128, 256), BF16), vm((KW, 2, 128, 256), F32), vm((2, KW, 128, 256), F32),
        vm((8, 128), F32),
        vm((128, 512), BF16), vm((128, 512), BF16), vm((2, 2, 128, 512), BF16), vm((128, 1024), BF16),
        vm((npos, nsg * cw // 2, 128), BF16), vm((npos, 2, nsg * cw // 2, 128), BF16),
        vm((nsg, cw, 1024), BF16), vm((nsg, cw, 1024), BF16), vm((nsg * cw, 1024), F32),
        dma((16,)), dma((8,)), dma((8,)), dma((5,)), dma((8,)), dma((2,)), dma((3, 3)), dma((3, 8)),
        dma((4,)), dma((4,)), dma((KW, 3)), dma((KW, 8)), dma((3,)), dma((4,)),
        dma((KW, 2)), dma((KW, 2)), dma((4,)), dma((4,)), dma((8, 2)), dma((8, 2)), dma((8,)), dma((8,)),
    ]
    out_shape = (
        jax.ShapeDtypeStruct((KW, 128), F32),
        jax.ShapeDtypeStruct((128, 1024), BF16),
        jax.ShapeDtypeStruct((cw, 1024), F32),
    )
    hbm = pl.BlockSpec(memory_space=pl.ANY)
    vmem = pl.BlockSpec(memory_space=pltpu.VMEM)
    made = pl.pallas_call(
        functools.partial(kernel, seq_size),
        out_shape=out_shape,
        in_specs=[hbm] * 9,
        out_specs=(vmem, vmem, vmem),
        scratch_shapes=scratch,
        compiler_params=pltpu.CompilerParams(
            collective_id=0, has_side_effects=True, vmem_limit_bytes=60 * 2**20
        ),
        name="depth_window",
    )(
        hidden, w_proj, codes.T, embed_table, jnp.transpose(w_qkv, (1, 0, 2)), w_out, head_table,
        gain_attn.reshape(1, -1), gain_head.reshape(1, -1),
    )
    loss, grad_hidden, grad_proj = pl.pallas_call(
        hand_out, out_shape=out_shape, in_specs=[vmem] * 3, out_specs=(vmem,) * 3, name="hand_out"
    )(*made)
    return loss.T, grad_hidden, grad_proj.T


def solution(mesh):
    return jax.shard_map(
        body,
        mesh=mesh,
        in_specs=(
            P("seq", "tp"),
            P("tp", None),
            P("seq", None),
            P(None, None, "tp"),
            P(None, None, "tp"),
            P("tp", None),
            P(None, None, "tp"),
            P(),
            P(),
        ),
        out_specs=(P("seq", None), P("seq", "tp"), P("tp", "seq")),
        check_vma=False,
    )
```

```python
import functools

import jax
import jax.numpy as jnp
from jax import lax
from jax.experimental import pallas as pl
from jax.experimental.pallas import tpu as pltpu
from jax.sharding import PartitionSpec as P

HEADS = 16
KW = 4
TP = 4
EPS = 1e-06
RB = 32
WCUT = 192
F32 = jnp.float32
BF16 = jnp.bfloat16
MESH = pl.DeviceIdType.MESH
LAYOUT = {64: (2, 8, 4), 8: (2, 2, 2)}


def mm(a, b):
    return jnp.dot(a, b, preferred_element_type=F32)


def mm_t(a, b):
    return lax.dot_general(a, b, (((1,), (1,)), ((), ())), preferred_element_type=F32)


def remote(src, dst, send, recv, device):
    return pltpu.make_async_remote_copy(
        src_ref=src, dst_ref=dst, send_sem=send, recv_sem=recv, device_id=device, device_id_type=MESH
    )


def kernel(
    seq_size,
    hid_h, wproj_h, codes_h, emb_h, wqkv_h, wo_h, head_h, ga_h, gh_h,
    loss_o, ghid_o, gproj_o,
    hg, wproj, codes, emb, wqkv, wo, head, ga, gh,
    ccol, looked, c_s, c_r, c_2, s_in, s_mid, normed, q, k, v, wts, att, bd,
    big, g1, g2, ep, r_in, r_mid, st_c, st, sc, midsum, b_s, b_r, b_s2, b_r2, ag, dkv, dqkv,
    e_s, e_r, e_2, cg, tsend, trecv, psend, precv, part,
    lsem, hid_ss, hid_rs, wo_ss, wo_rs, wo_q, lk_ss, lk_rs, c_ss, c_rs, att_ss, att_rs,
    st_ss, st_rs, b_ss, b_rs, e_ss, e_rs, t_ss, t_rs, p_ss, p_rs,
):
    xs, zs, ys = LAYOUT[seq_size]
    zb_n = min(2, zs)
    zh_n = zs // zb_n
    npos, nsg = zb_n * ys, xs * zh_n
    cw = 1024 // seq_size
    total = float(128 * seq_size * KW)

    r = lax.axis_index("tp")
    s = lax.axis_index("seq")
    core = r % 2
    chip = r // 2
    p = chip * 2 + (1 - core)
    x = (1 - chip) * 2 + core
    d = (1 - chip) * 2 + (1 - core)
    y = s % ys
    z = (s // ys) % zs
    xh = s // (ys * zs)
    pos = (z % zb_n) * ys + y
    sg = xh * zh_n + z // zb_n
    to_p, to_x, to_d = {"tp": p}, {"tp": x}, {"tp": d}
    flip = {"seq": (xs - 1 - xh) * (ys * zs) + z * ys + y, "tp": x}

    def seq_of(position, supergroup):
        yy, zb = position % ys, position // ys
        zh, xx = supergroup % zh_n, supergroup // zh_n
        return xx * (ys * zs) + (zh * zb_n + zb) * ys + yy

    def around(size):
        return sorted(range(size), key=lambda i: -min(i, size - i))

    pos_peers = [
        lax.rem(z + n, 2) * ys + lax.rem(y + m, ys) for m in around(ys) for n in (1, 0) if n or m
    ]
    sg_peers = [
        lax.rem(xh + n, xs) * zh_n + lax.rem(z // zb_n + m, zh_n) for m in around(zh_n) for n in (1, 0) if n or m
    ]

    def load(src, dst, i):
        copy = pltpu.make_async_copy(src, dst, lsem.at[i])
        copy.start()
        return copy

    l_hid = load(hid_h, hg.at[pos], 0)
    l_wproj = load(wproj_h, wproj, 1)
    l_codes = load(codes_h, codes, 2)
    l_emb = [load(emb_h.at[i], emb.at[i], 3 + i) for i in range(3)]
    l_ga = load(ga_h, ga, 6)
    l_gh = load(gh_h, gh, 7)
    l_qkv = load(wqkv_h, wqkv, 8)
    l_wo = load(wo_h, wo.at[r], 9)
    l_head = load(head_h, head, 10)

    barrier = pltpu.get_barrier_semaphore()
    peers = [to_p, to_x, to_d, flip]
    peers += [{"seq": seq_of(i, sg)} for i in pos_peers]
    peers += [{"seq": seq_of(i, sg), "tp": p} for i in pos_peers]
    peers += [{"seq": seq_of(pos, i)} for i in sg_peers]
    for peer in peers:
        pl.semaphore_signal(barrier, inc=1, device_id=peer, device_id_type=MESH)

    lane = lax.broadcasted_iota(jnp.int32, (128, 128), 1)
    bd[...] = (
        lax.broadcasted_iota(jnp.int32, (256, 256), 0) // 64
        == lax.broadcasted_iota(jnp.int32, (256, 256), 1) // 64
    ).astype(F32).astype(BF16)
    l_codes.wait()
    st_c[...] = jnp.zeros_like(st_c)
    st_c[0:KW, :] = codes[...].astype(F32)
    code_cols = st_c[...].T
    for i in range(KW):
        ccol[i] = jnp.broadcast_to(code_cols[:, i : i + 1], (128, 128)).astype(jnp.int32)
    l_hid.wait()
    l_wproj.wait()
    mine = pl.ds(pl.multiple_of(core * 512, 512), 512)
    other = pl.ds(pl.multiple_of((1 - core) * 512, 512), 512)
    c_s[...] = mm(hg[pos], wproj[:, other]).astype(BF16)
    big[:, 0:512] = mm(hg[pos], wproj[:, mine])

    def look_up(i):
        l_emb[i].wait()
        code = ccol[i]
        hot = jnp.concatenate(
            [(code == lane + 128 * g).astype(F32).astype(BF16) for g in range(16)], axis=1
        )
        looked[r, i] = mm(hot, emb[i]).astype(BF16)

    look_up(0)

    pl.semaphore_wait(barrier, len(peers))

    relays = []

    def send(src, dst, ss, rs, to):
        copy = remote(src, dst, ss, rs, to)
        copy.start()
        relays.append(copy)

    def relay(buf, ss, rs):
        send(buf, buf, ss, rs, to_p)

    def landed(buf, recv):
        remote(buf, buf, lsem.at[15], recv, to_p).wait_recv()

    def look(i, n):
        send(looked.at[r, i], looked.at[r, i], lk_ss.at[i, n], lk_rs.at[i, r], (to_x, to_p)[n])

    send(wo_h.at[0:WCUT], wo.at[r, 0:WCUT], wo_ss.at[1], wo_rs.at[r], flip)
    c1 = remote(c_s, c_r, c_ss.at[0], c_rs.at[0], to_p)
    c1.start()
    look(0, 0)
    look_up(1)
    c1.wait_recv()
    c_2[chip, core] = (big[:, 0:512] + c_r[...].astype(F32)).astype(BF16)
    send(c_2.at[chip, core], c_2.at[chip, core], c_ss.at[1], c_rs.at[1], to_x)
    send(c_2.at[chip, core], c_2.at[chip, core], c_ss.at[2], c_rs.at[2], to_p)
    look(1, 0)
    look(0, 1)
    look(1, 1)
    look_up(2)
    look(2, 0)
    look(2, 1)
    send(wo_h.at[WCUT:256], wo.at[r, WCUT:256], wo_ss.at[3], wo_q.at[0], to_x)
    send(wo_h, wo.at[r], wo_ss.at[0], wo_rs.at[r], to_p)

    for n in range(1, ys):
        py = lax.rem(y + n, ys)
        send(hid_h, hg.at[pos], hid_ss.at[n - 1], hid_rs.at[pos], {"seq": seq_of((z % zb_n) * ys + py, sg)})
    pos_z = (1 - z % zb_n) * ys + y
    send(hid_h, hg.at[pos], hid_ss.at[3], hid_rs.at[pos], {"seq": seq_of(pos_z, sg)})

    def vocab_hit(i):
        code = ccol[i]
        return jnp.concatenate([code == lane + (128 * g + r * 512) for g in range(4)], axis=1)

    def hot_product(i):
        g2[i] = mm_t(vocab_hit(i).astype(F32).astype(BF16), head[i]).astype(BF16)

    landed(looked.at[x, 0], lk_rs.at[0, x])
    relay(looked.at[x, 0], lk_ss.at[0, 2], lk_rs.at[0, x + 4])
    l_head.wait()
    hot_product(0)
    landed(c_2.at[1 - chip, core], c_rs.at[1])
    relay(c_2.at[1 - chip, core], c_ss.at[3], c_rs.at[3])
    hot_product(1)
    l_ga.wait()
    landed(c_2.at[chip, 1 - core], c_rs.at[2])
    landed(c_2.at[1 - chip, 1 - core], c_rs.at[3])

    def stream_rows(i):
        for rb in range(128 // RB):
            rows = slice(rb * RB, (rb + 1) * RB)
            ctx = jnp.concatenate(
                [c_2[0, h, rows, :].astype(F32) + c_2[1, h, rows, :].astype(F32) for h in range(2)], axis=1
            )
            if i > 0:
                ctx = ctx + jnp.concatenate([looked[j, i - 1, rows, :].astype(F32) for j in range(TP)], axis=1)
            s_in[i, rows, :] = ctx
            scale = lax.rsqrt(jnp.mean(ctx * ctx, axis=1, keepdims=True) + EPS)
            r_in[i, rows, :] = jnp.broadcast_to(scale, (RB, 128))
            normed[i, rows, :] = (ctx * scale * ga[...]).astype(BF16)

    def project(i):
        for n, dst in enumerate((q, k, v)):
            dst[i] = mm(normed[i], wqkv[n]).astype(BF16)

    def attend(a):
        probe = [q[a].astype(F32) * k[b].astype(F32) for b in range(a + 1)]
        if a == 0:
            att[r, 0] = v[0]
        else:
            prod = jnp.concatenate(probe, axis=0)
            high = prod.astype(BF16)
            low = (prod - high.astype(F32)).astype(BF16)
            sums = (mm(high, bd[...]) + mm(low, bd[...])) * 0.125
            rows = [sums[b * 128 : (b + 1) * 128] for b in range(a + 1)]
            top = functools.reduce(jnp.maximum, rows)
            rows = [jnp.exp(row - top) for row in rows]
            inv = 1.0 / functools.reduce(jnp.add, rows)
            out = jnp.zeros((128, 256), F32)
            for b in range(a + 1):
                w = rows[b] * inv
                wts[a * (a + 1) // 2 + b] = w
                out = out + w.astype(BF16).astype(F32) * v[b].astype(F32)
            att[r, a] = out.astype(BF16)
        for n, to in enumerate((to_x, to_p)):
            send(att.at[r, a], att.at[r, a], att_ss.at[a, n], att_rs.at[a, r], to)

    for i in range(KW):
        if i > 0:
            if i > 1:
                landed(looked.at[x, i - 1], lk_rs.at[i - 1, x])
                relay(looked.at[x, i - 1], lk_ss.at[i - 1, 2], lk_rs.at[i - 1, x + 4])
                hot_product(i)
            landed(looked.at[p, i - 1], lk_rs.at[i - 1, p])
            landed(looked.at[d, i - 1], lk_rs.at[i - 1, d + 4])
        stream_rows(i)
        if i == 0:
            l_qkv.wait()
        project(i)
        attend(i)

    landed(hg.at[pos_z], hid_rs.at[pos_z])
    for n in range(1, ys):
        py = lax.rem(y + n, ys)
        send(hg.at[pos_z], hg.at[pos_z], hid_ss.at[3 + n], hid_rs.at[pos_z], {"seq": seq_of((z % zb_n) * ys + py, sg)})
    l_wo.wait()
    for i in range(KW):
        s_mid[i] = s_in[i] + mm(att[r, i], wo[r])
    landed(wo.at[p], wo_rs.at[p])
    for i in range(KW):
        landed(att.at[p, i], att_rs.at[i, p])
        s_mid[i] = s_mid[i] + mm(att[p, i], wo[p])
    landed(wo.at[x, 0:WCUT], wo_rs.at[x])
    relay(wo.at[x, 0:WCUT], wo_ss.at[2], wo_rs.at[x + 4])
    landed(wo.at[x, WCUT:256], wo_q.at[0])
    relay(wo.at[x, WCUT:256], wo_ss.at[4], wo_q.at[1])
    l_gh.wait()
    midsum[...] = jnp.zeros_like(midsum)

    def norm_mid(i):
        for rb in range(128 // RB):
            rows = slice(rb * RB, (rb + 1) * RB)
            val = s_mid[i, rows, :]
            scale = lax.rsqrt(jnp.mean(val * val, axis=1, keepdims=True) + EPS)
            r_mid[i, rows, :] = jnp.broadcast_to(scale, (RB, 128))
            normed[i, rows, :] = (val * scale * gh[...]).astype(BF16)

    def heads(i):
        logits = mm(normed[i], head[i])
        hit = vocab_hit(i)
        top = jnp.max(logits, axis=1, keepdims=True)
        grown = jnp.exp(logits - top)
        total_exp = jnp.sum(grown, axis=1, keepdims=True)
        target = jnp.sum(jnp.where(hit, logits, 0.0), axis=1, keepdims=True)
        ep[i] = jnp.where(hit, 0.0, grown).astype(BF16)
        return top, total_exp, target

    found = []
    for pair in ((0, 1), (2, 3)):
        for i in pair:
            landed(att.at[x, i], att_rs.at[i, x])
            relay(att.at[x, i], att_ss.at[i, 2], att_rs.at[i, x + 4])
        for i in pair:
            s_mid[i] = s_mid[i] + mm(att[x, i], wo[x])
        if pair[0] == 0:
            landed(wo.at[d, 0:WCUT], wo_rs.at[d + 4])
            landed(wo.at[d, WCUT:256], wo_q.at[1])
        for i in pair:
            landed(att.at[d, i], att_rs.at[i, d + 4])
        for i in pair:
            s_mid[i] = s_mid[i] + mm(att[d, i], wo[d])
        for i in pair:
            norm_mid(i)
        found += [heads(i) for i in pair]
    rows_st = jnp.zeros((128, 128), F32)
    for i in range(KW):
        for n in range(3):
            rows_st = jnp.where(lane == i + 8 * n, found[i][n], rows_st)
    st_c[...] = rows_st
    st[r] = st_c[...].T[0:24, :]
    stats = []
    for n, to in enumerate((to_p, to_x, to_d)):
        copy = remote(st.at[r], st.at[r], st_ss.at[n], st_rs.at[r], to)
        copy.start()
        stats.append(copy)
    for i in range(KW):
        g1[i] = mm_t(ep[i], head[i])
    for slot in (p, x, d):
        landed(st.at[slot], st_rs.at[slot])
    tops = [st[j, 0:8, :] for j in range(TP)]
    top = functools.reduce(jnp.maximum, tops)
    exp_total = functools.reduce(jnp.add, [st[j, 8:16, :] * jnp.exp(tops[j] - top) for j in range(TP)])
    target = functools.reduce(jnp.add, [st[j, 16:24, :] for j in range(TP)])
    log_total = top + jnp.log(exp_total)
    loss_o[...] = (log_total - target)[0:KW, :]
    sc[...] = jnp.zeros_like(sc)
    sc[0:8, :] = jnp.exp(st[r, 0:8, :] - log_total) * (1.0 / total)
    sc[8:16, :] = (jnp.exp(target - log_total) - 1.0) * (1.0 / total)
    sc[...] = sc[...].T

    def send_on(i):
        landed(b_r.at[i], b_rs.at[i, 0])
        b_s2[i] = (ag[i, 1] + b_r[i, 1].astype(F32)).astype(BF16)
        remote(b_s2.at[i], b_r2.at[i], b_ss.at[i, 1], b_rs.at[i, 1], to_x).start()

    def head_rows(i):
        for rb in range(128 // RB):
            rows = slice(rb * RB, (rb + 1) * RB)
            grow = sc[rows, i : i + 1]
            hot = sc[rows, i + 8 : i + 9]
            val = s_mid[i, rows, :]
            cot = (grow * g1[i, rows, :] + hot * g2[i, rows, :].astype(F32)) * gh[...]
            scale = r_mid[i, rows, 0:1]
            along = jnp.mean(cot * val, axis=1, keepdims=True) * (scale * scale * scale)
            back = cot * scale - val * along
            midsum[rows, :] = midsum[rows, :] + back
            normed[i, rows, :] = back.astype(BF16)

    head_rows(KW - 1)
    for i in range(KW - 1, -1, -1):
        b_s[i, 0] = mm_t(normed[i], wo[p]).astype(BF16)
        b_s[i, 1] = mm_t(normed[i], wo[d]).astype(BF16)
        remote(b_s.at[i], b_r.at[i], b_ss.at[i, 0], b_rs.at[i, 0], to_p).start()
        if i < KW - 1:
            send_on(i + 1)
        ag[i, 1] = mm_t(normed[i], wo[x])
        ag[i, 0] = mm_t(normed[i], wo[r])
        if i > 0:
            head_rows(i - 1)
    send_on(0)

    for a in range(KW - 1, -1, -1):
        landed(b_r2.at[a], b_rs.at[a, 1])
        out_grad = (ag[a, 0] + b_r[a, 0].astype(F32) + b_r2[a].astype(F32)).astype(BF16).astype(F32)
        if a == 0:
            dq = jnp.zeros((128, 256), F32)
            dk = dkv[0, 0]
            dv = dkv[1, 0] + out_grad
        else:
            prod = jnp.concatenate([out_grad * v[b].astype(F32) for b in range(a + 1)], axis=0)
            high = prod.astype(BF16)
            low = (prod - high.astype(F32)).astype(BF16)
            sums = mm(high, bd[...]) + mm(low, bd[...])
            base = a * (a + 1) // 2
            grads = [sums[b * 128 : (b + 1) * 128] for b in range(a + 1)]
            inner = functools.reduce(jnp.add, [wts[base + b] * grads[b] for b in range(a + 1)])
            dq = jnp.zeros((128, 256), F32)
            for b in range(a + 1):
                w = wts[base + b]
                sgrad = (w * (grads[b] - inner) * 0.125).astype(BF16).astype(F32)
                dq = dq + sgrad * k[b].astype(F32)
                dk_b = sgrad * q[a].astype(F32)
                dv_b = w.astype(BF16).astype(F32) * out_grad
                if a == KW - 1:
                    dkv[0, b] = dk_b
                    dkv[1, b] = dv_b
                else:
                    dkv[0, b] = dkv[0, b] + dk_b
                    dkv[1, b] = dkv[1, b] + dv_b
            dk = dkv[0, a]
            dv = dkv[1, a]
        big[...] = (
            mm_t(dq.astype(BF16), wqkv[0]) + mm_t(dk.astype(BF16), wqkv[1]) + mm_t(dv.astype(BF16), wqkv[2])
        )

        for rb in range(128 // RB):
            rows = slice(rb * RB, (rb + 1) * RB)
            val = s_in[a, rows, :]
            cot = big[rows, :] * ga[...]
            scale = r_in[a, rows, 0:1]
            along = jnp.mean(cot * val, axis=1, keepdims=True) * (scale * scale * scale)
            midsum[rows, :] = midsum[rows, :] + cot * scale - val * along

    e_s[...] = midsum[:, other].astype(BF16)
    e1 = remote(e_s, e_r, e_ss.at[0], e_rs.at[0], to_p)
    e1.start()
    e1.wait_recv()
    e_2[chip, core] = (midsum[:, mine] + e_r[...].astype(F32)).astype(BF16)
    e2x = remote(e_2.at[chip, core], e_2.at[chip, core], e_ss.at[1], e_rs.at[1], to_x)
    e2p = remote(e_2.at[chip, core], e_2.at[chip, core], e_ss.at[2], e_rs.at[2], to_p)
    e2x.start()
    e2p.start()
    landed(e_2.at[1 - chip, core], e_rs.at[1])
    relay(e_2.at[1 - chip, core], e_ss.at[3], e_rs.at[3])

    cg[:, mine] = (e_2[0, core].astype(F32) + e_2[1, core].astype(F32)).astype(BF16)
    for j in range(4):
        block = (
            e_2[0, core, :, j * 128 : (j + 1) * 128].astype(F32) + e_2[1, core, :, j * 128 : (j + 1) * 128].astype(F32)
        ).T.astype(BF16)
        for m in range(128 // cw):
            owner = j * (128 // cw) + m
            yy, zz = owner % ys, owner // ys
            at = (zz // zb_n) * cw
            tsend[(zz % zb_n) * ys + yy, at : at + cw, :] = block[m * cw : (m + 1) * cw]
    for n, peer in enumerate(pos_peers):
        for m, to in enumerate((r, p)):
            send(tsend.at[peer], trecv.at[pos, core], t_ss.at[n, m], t_rs.at[pos, core], {"seq": seq_of(peer, sg), "tp": to})
    send(tsend.at[pos], trecv.at[pos, core], t_ss.at[7, 0], t_rs.at[pos, core], to_p)
    trecv[pos, core] = tsend[pos]

    landed(e_2.at[chip, 1 - core], e_rs.at[2])
    landed(e_2.at[1 - chip, 1 - core], e_rs.at[3])
    cg[:, other] = (e_2[0, 1 - core].astype(F32) + e_2[1, 1 - core].astype(F32)).astype(BF16)
    for n in range(4):
        cols = slice(n * 256, (n + 1) * 256)
        ghid_o[:, cols] = mm_t(cg[...], wproj[cols, :]).astype(BF16)

    for n in range(1, npos):
        slot = lax.rem(pos + n, npos)

        @pl.when(slot != pos_z)
        def _():
            landed(hg.at[slot], hid_rs.at[slot])

    landed(trecv.at[pos, 1 - core], t_rs.at[pos, 1 - core])
    part[...] = mm(trecv[pos].reshape(nsg * cw, 128), hg[pos])
    for peer in pos_peers:
        landed(trecv.at[peer, core], t_rs.at[peer, core])
        landed(trecv.at[peer, 1 - core], t_rs.at[peer, 1 - core])
        part[...] = part[...] + mm(trecv[peer].reshape(nsg * cw, 128), hg[peer])
    for n in range(nsg):
        psend[n] = part[n * cw : (n + 1) * cw, :].astype(BF16)
    for n, peer in enumerate(sg_peers):
        send(psend.at[peer], precv.at[sg], p_ss.at[n], p_rs.at[sg], {"seq": seq_of(pos, peer)})
    precv[sg] = psend[sg]
    for peer in sg_peers:
        landed(precv.at[peer], p_rs.at[peer])
    gproj_o[...] = functools.reduce(jnp.add, [precv[n].astype(F32) for n in range(nsg)])

    for copy in (c1, e1, e2x, e2p, *relays, *stats):
        copy.wait_send()
    for i in range(KW):
        remote(b_s.at[i], b_r.at[i], b_ss.at[i, 0], b_rs.at[i, 0], to_p).wait_send()
        remote(b_s2.at[i], b_r2.at[i], b_ss.at[i, 1], b_rs.at[i, 1], to_x).wait_send()


def hand_out(loss_i, ghid_i, gproj_i, loss_o, ghid_o, gproj_o):
    loss_o[...] = loss_i[...]
    ghid_o[...] = ghid_i[...]
    gproj_o[...] = gproj_i[...]


def body(hidden, w_proj, codes, embed_table, w_qkv, w_out, head_table, gain_attn, gain_head):
    seq_size = lax.axis_size("seq")
    xs, zs, ys = LAYOUT[seq_size]
    npos = min(2, zs) * ys
    nsg = seq_size // npos
    cw = 1024 // seq_size
    vm, dma = pltpu.VMEM, pltpu.SemaphoreType.DMA
    scratch = [
        vm((npos, 128, 1024), BF16), vm((1024, 1024), BF16), vm((KW, 128), jnp.int32),
        vm((3, 2048, 256), BF16), vm((3, 1024, 256), BF16), vm((TP, 256, 1024), BF16),
        vm((KW, 1024, 512), BF16), vm((1, 1024), F32), vm((1, 1024), F32),
        vm((KW, 128, 128), jnp.int32), vm((TP, 3, 128, 256), BF16),
        vm((128, 512), BF16), vm((128, 512), BF16), vm((2, 2, 128, 512), BF16),
        vm((KW, 128, 1024), F32), vm((KW, 128, 1024), F32), vm((KW, 128, 1024), BF16),
        vm((KW, 128, 256), BF16), vm((KW, 128, 256), BF16), vm((KW, 128, 256), BF16),
        vm((10, 128, 256), F32), vm((TP, KW, 128, 256), BF16), vm((256, 256), BF16),
        vm((128, 1024), F32), vm((KW, 128, 1024), F32), vm((KW, 128, 1024), BF16),
        vm((KW, 128, 512), BF16), vm((KW, 128, 128), F32), vm((KW, 128, 128), F32), vm((128, 128), F32),
        vm((TP, 24, 128), F32), vm((128, 128), F32), vm((128, 1024), F32),
        vm((KW, 2, 128, 256), BF16), vm((KW, 2, 128, 256), BF16), vm((KW, 128, 256), BF16),
        vm((KW, 128, 256), BF16), vm((KW, 2, 128, 256), F32), vm((2, KW, 128, 256), F32),
        vm((8, 128), F32),
        vm((128, 512), BF16), vm((128, 512), BF16), vm((2, 2, 128, 512), BF16), vm((128, 1024), BF16),
        vm((npos, nsg * cw // 2, 128), BF16), vm((npos, 2, nsg * cw // 2, 128), BF16),
        vm((nsg, cw, 1024), BF16), vm((nsg, cw, 1024), BF16), vm((nsg * cw, 1024), F32),
        dma((16,)), dma((8,)), dma((8,)), dma((5,)), dma((8,)), dma((2,)), dma((3, 3)), dma((3, 8)),
        dma((4,)), dma((4,)), dma((KW, 3)), dma((KW, 8)), dma((3,)), dma((4,)),
        dma((KW, 2)), dma((KW, 2)), dma((4,)), dma((4,)), dma((8, 2)), dma((8, 2)), dma((8,)), dma((8,)),
    ]
    out_shape = (
        jax.ShapeDtypeStruct((KW, 128), F32),
        jax.ShapeDtypeStruct((128, 1024), BF16),
        jax.ShapeDtypeStruct((cw, 1024), F32),
    )
    hbm = pl.BlockSpec(memory_space=pl.ANY)
    vmem = pl.BlockSpec(memory_space=pltpu.VMEM)
    made = pl.pallas_call(
        functools.partial(kernel, seq_size),
        out_shape=out_shape,
        in_specs=[hbm] * 9,
        out_specs=(vmem, vmem, vmem),
        scratch_shapes=scratch,
        compiler_params=pltpu.CompilerParams(
            collective_id=0, has_side_effects=True, vmem_limit_bytes=60 * 2**20
        ),
        name="depth_window",
    )(
        hidden, w_proj, codes.T, embed_table, jnp.transpose(w_qkv, (1, 0, 2)), w_out, head_table,
        gain_attn.reshape(1, -1), gain_head.reshape(1, -1),
    )
    loss, grad_hidden, grad_proj = pl.pallas_call(
        hand_out, out_shape=out_shape, in_specs=[vmem] * 3, out_specs=(vmem,) * 3, name="hand_out"
    )(*made)
    return loss.T, grad_hidden, grad_proj.T


def solution(mesh):
    return jax.shard_map(
        body,
        mesh=mesh,
        in_specs=(
            P("seq", "tp"),
            P("tp", None),
            P("seq", None),
            P(None, None, "tp"),
            P(None, None, "tp"),
            P("tp", None),
            P(None, None, "tp"),
            P(),
            P(),
        ),
        out_specs=(P("seq", None), P("seq", "tp"), P("tp", "seq")),
        check_vma=False,
    )
```
